256 devices in a mesh: rep: 2 (over core), tab: 128 (over y, z, x).
Axes of the slice: x: 4, y: 4, z: 8, core: 2. Of those that a mesh axis runs over, the one named last changes fastest.
Arguments:
- grad_out: bfloat16 [65536, 128, 128], P(('rep', 'tab')), may hold values from -1.5 to 1.5
- indices: int32 [128, 65536], P('tab', 'rep'), may hold values from 0 to 1023
- projections: bfloat16 [128, 128, 128], P('tab'), may hold values from -0.75 to 0.75
- widths: int32 [128], replicated, may hold values from 16 to 128
- hot_ids: int32 [128, 32], P('tab'), may hold values from 0 to 1023, as said below
Outputs:
- cold_grad: float32 [2, 128, 1024, 128], P('rep', 'tab')
- hot_grad: float32 [128, 32, 128], P('tab', 'rep')
The draws below stay inside these ranges and needn't reach their ends.
Inputs may be any that keep to these rules, and one draw needn't show every extreme that they name: `hot_ids`: the 32 hot rows of one table are distinct.
All inputs are finite; a program needn't handle non-finite values.
Results may differ from the reference program's by a relative error of at most 0.005.
Values may be sent and summed in bfloat16 or wider, within the bound.
A program may use at most 128 MiB of HBM per device.

```python
import jax
import jax.numpy as jnp
from jax import lax

BASE = 128
ROWS = 1024
HOT = 32
NT = 128
HALF = 32768
BATCH = 65536
N_REP = 2


def shared_hot(key):
    table_keys = jax.random.split(jax.random.fold_in(key, 7), NT)
    return jax.vmap(lambda table_key: jax.random.permutation(table_key, ROWS)[:HOT])(table_keys).astype(jnp.int32)


def draw_hot_ids(key, part):
    return shared_hot(key)


def draw_indices(key, part):
    hot_rows = shared_hot(key)
    pick_key = jax.random.fold_in(key, 11)
    cold_key = jax.random.fold_in(key, 13)
    use_key = jax.random.fold_in(key, 17)
    pick = jax.random.randint(pick_key, (NT, BATCH), 0, HOT, dtype=jnp.int32)
    drawn = jax.random.randint(cold_key, (NT, BATCH), 0, ROWS, dtype=jnp.int32)
    use_hot = jax.random.randint(use_key, (NT, BATCH), 0, 8, dtype=jnp.int32) == 0
    chosen = jnp.take_along_axis(hot_rows, pick, axis=1)
    return jnp.where(use_hot, chosen, drawn).astype(jnp.int32)


def plant(result, stream_key, low, top_value):
    dims = result.shape
    place = [jax.random.randint(jax.random.fold_in(stream_key, axis), (), 0, dims[axis]) for axis in range(len(dims))]
    result = result.at[tuple(place)].set(low)
    longest = dims.index(max(dims))
    place[longest] = (place[longest] + 1) % dims[longest]
    return result.at[tuple(place)].set(top_value)


def levels(own_key, extent, cuts, smallest, largest):
    def one(dim, shards_of):
        draws = jax.random.uniform(jax.random.fold_in(jax.random.fold_in(own_key, 6), dim), (shards_of,), jnp.float32, smallest / len(cuts), largest / len(cuts))
        return jnp.repeat(jnp.exp(draws), extent[dim] // shards_of).reshape((-1,) + (1,) * (len(extent) - dim - 1))

    level = one(*cuts[0])
    for cut in cuts[1:]:
        level = level * one(*cut)
    return level


def gaussian(key, shape, scale, reach, shards=(), kind=jnp.bfloat16):
    level = levels(key, shape, shards, -0.22, 0.18) if shards else 1.0
    drawn = jax.random.normal(key, shape, jnp.float32) * scale * level
    return jnp.minimum(jnp.maximum(drawn, -reach), reach).astype(kind)


def setup_inputs(seed: int = 0) -> dict:
    streams_of = jax.random.split(jax.random.key(seed), 6)
    grad_out = gaussian(streams_of[0], (BATCH, NT, BASE), 0.25, 1.5, ((0, 256),))
    indices = draw_indices(jax.random.fold_in(streams_of[5], 71), 0)
    projections = gaussian(streams_of[2], (NT, BASE, BASE), (BASE // 2) ** -0.5, 0.75, ((0, 128),))
    widths = plant(jax.random.randint(streams_of[3], (NT,), BASE // 8, BASE + 1), jax.random.fold_in(streams_of[3], 1), BASE // 8, BASE).astype(jnp.int32)
    hot_ids = draw_hot_ids(jax.random.fold_in(streams_of[5], 71), 0)
    return {"grad_out": grad_out, "indices": indices, "projections": projections, "widths": widths, "hot_ids": hot_ids}


def reference(grad_out, indices, projections, widths, hot_ids):
    columns = jnp.arange(BASE, dtype=jnp.int32)
    all_rows = jnp.arange(ROWS, dtype=jnp.int32)

    def one_table(packed):
        table, lookups, project_w, width, hot_rows = packed
        grads = lax.dynamic_index_in_dim(grad_out, table, 1, keepdims=False)
        full_proj = jnp.dot(grads, project_w, preferred_element_type=jnp.float32)
        projected = jnp.where(columns[None, :] < width, full_proj, 0.0).astype(jnp.bfloat16)
        halves_proj = projected.reshape(N_REP, HALF, BASE)
        halves_rows = lookups.reshape(N_REP, HALF)
        row_grads = jnp.stack([jax.ops.segment_sum(halves_proj[half].astype(jnp.float32), halves_rows[half], num_segments=ROWS) for half in range(N_REP)])
        picked = row_grads[:, hot_rows, :]
        hot_sum = picked[0] + picked[1]
        is_hot = jnp.any(hot_rows[:, None] == all_rows[None, :], axis=0)
        cold_rows = jnp.where(is_hot[None, :, None], jnp.float32(0.0), row_grads)
        return cold_rows, hot_sum

    tables = jnp.arange(NT, dtype=jnp.int32)
    cold_all, hot_all = lax.map(one_table, (tables, indices, projections, widths, hot_ids))
    return jnp.swapaxes(cold_all, 0, 1), hot_all
```

```python
import jax
import jax.numpy as jnp
from jax import lax
from jax.experimental import pallas as pl
from jax.experimental.pallas import tpu as pltpu
from jax.sharding import PartitionSpec as P

ROWS = 1024
NX, NY, NZ = 4, 4, 8
STEPS = 4
F32 = jnp.float32
BF16 = jnp.bfloat16


def kernel(grad_ref, idx_ref, proj_ref, widths_ref, hot_ref, cold_ref, hotout_ref,
           stage, tmp, turn, raw, fsum, own, part, leaf, near, zsend, zrecv,
           zi, pi, hot_all, hot_got,
           load_sem, raw_s, raw_r, leaf_s, leaf_r, near_s, near_r, z_s, z_r,
           iz_s, iz_r, iq_s, iq_r, hot_s, hot_r):
    rep = lax.axis_index("rep")
    tab = lax.axis_index("tab")
    x = tab % NX
    z = (tab // NX) % NZ
    y = tab // (NX * NZ)

    def at(px, py, pz):
        return {"tab": (py * NZ + pz) * NX + px}

    def peer(mode, along, shift):
        on_y = (1 - along) * (1 - mode) + along * mode
        return at((x + (1 - on_y) * shift) % NX, (y + on_y * shift) % NY, z)

    def remote(src, dst, s, r, dev):
        return pltpu.make_async_remote_copy(
            src_ref=src, dst_ref=dst, send_sem=s, recv_sem=r,
            device_id=dev, device_id_type=pl.DeviceIdType.MESH)

    def pair_of(step):
        return (z // 2 + 2 + 3 * step + (step // 2) * (3 - 2 * (step % 2))) % 4

    def load(step, d):
        tile = ((y + d) % NY) * 4 + pair_of(step)
        return pltpu.make_async_copy(
            grad_ref.at[:, pl.ds(pl.multiple_of(tile * 8, 8), 8), :],
            stage.at[step, d], load_sem.at[step, d])

    def start_loads(i, c):
        load(i // 4, i % 4).start()
        return c

    lax.fori_loop(0, 16, start_loads, 0)

    barrier = pltpu.get_barrier_semaphore()

    def greet(dev):
        pl.semaphore_signal(barrier, inc=1, device_id=dev, device_id_type=pl.DeviceIdType.MESH)

    for d in range(1, 4):
        greet(at((x + d) % NX, y, z))
        greet(at(x, (y + d) % NY, z))
    for d in range(1, 8):
        greet(at(x, y, (z + d) % NZ))
    greet({"rep": 1 - rep})
    pl.semaphore_wait(barrier, 14)

    def iz(d):
        to = (z + d) % NZ
        return remote(idx_ref.at[to], zi.at[z % 2, z // 2], iz_s.at[d - 1], iz_r.at[d - 1], at(x, y, to))

    for d in range(1, 8):
        iz(d).start()
    zi[z % 2, z // 2] = idx_ref[z]

    def raw_copy(mode, step, d):
        pos = y * (1 - mode) + x * mode
        return remote(turn.at[mode, step, (pos + d) % 4], raw.at[mode, step, d - 1],
                      raw_s.at[mode, step, d - 1], raw_r.at[mode, step, d - 1], peer(mode, 0, d))

    def relayout(step):
        def one(d, c):
            load(step, d).wait()
            tmp[...] = stage[step, d].astype(F32).reshape(2048, 128)
            to_y = (y + d) % NY
            for px in range(4):
                turn[0, step, to_y, px] = tmp[pl.ds(px, 256, stride=8), :].astype(BF16)
            for px in range(4):
                turn[1, step, px, to_y] = tmp[pl.ds(4 + px, 256, stride=8), :].astype(BF16)
            return c

        lax.fori_loop(0, 4, one, 0)

        def send(i, c):
            raw_copy(i % 2, step, i // 2 + 1).start()
            return c

        lax.fori_loop(0, 6, send, 0)

    relayout(0)

    def iq(mode, d):
        pos = x * (1 - mode) + y * mode
        return remote(zi.at[mode, :, (pos + d) % 4], pi.at[mode, :, pos],
                      iq_s.at[mode, d - 1], iq_r.at[mode, d - 1], peer(mode, 1, d))

    for d in range(1, 8):
        iz(d).wait()
    for mode in range(2):
        for d in range(1, 4):
            iq(mode, d).start()
    pi[0, :, x] = zi[0, :, x]
    pi[1, :, y] = zi[1, :, y]
    for mode in range(2):
        for d in range(1, 4):
            iq(mode, d).wait()

    rows = lax.broadcasted_iota(jnp.int32, (ROWS, 128), 0)

    def onehot(ids, src):
        halves = []
        for h in range(2):
            line = pi[ids + (pl.ds(2 * src + h, 1), slice(None))]
            halves.append(jnp.where(rows == line, F32(1), F32(0)).astype(BF16))
        return jnp.concatenate(halves, axis=1)

    def table_sum(mode, step, dest):
        pos = y * (1 - mode) + x * mode
        ids = (mode, pair_of(step), dest)
        fsum[...] = jnp.dot(onehot(ids, pos), turn[mode, step, pos, dest], preferred_element_type=F32)

        def other(d, c):
            src = (pos + 4 - d) % 4
            fsum[...] += jnp.dot(onehot(ids, src), raw[mode, step, d - 1, dest], preferred_element_type=F32)
            return c

        lax.fori_loop(1, 4, other, 0)

    HALF = ROWS // 2

    def leaf_copy(mode, step, side):
        return remote(part.at[mode, step, 0, pl.ds(side * HALF, HALF)], leaf.at[mode, step, side],
                      leaf_s.at[mode, step, side], leaf_r.at[mode, step, side], peer(mode, 1, 1 + 2 * side))

    def near_copy(mode, step, side):
        return remote(part.at[mode, step, 1 + side], near.at[mode, step, side],
                      near_s.at[mode, step, side], near_r.at[mode, step, side], peer(mode, 1, 1 + 2 * side))

    def z_copy(mode, step):
        to = pair_of(step) * 2 + mode
        return remote(zsend.at[mode, step], zrecv.at[z], z_s.at[mode, step], z_r.at[z], at(x, y, to))

    def z_arrival(src):
        return remote(zsend.at[0, 0], zrecv.at[src], z_s.at[0, 0], z_r.at[src], at(x, y, src))

    def step_body(step, c):
        @pl.when(step < STEPS - 1)
        def _():
            relayout(step + 1)

        def arrive(i, c):
            raw_copy(i % 2, step, i // 2 + 1).wait_recv()
            return c

        lax.fori_loop(0, 6, arrive, 0)

        def table(i, c):
            mode = i % 2
            j = i // 2
            pos = x * (1 - mode) + y * mode
            shift = (2 + 2 * j + 3 * (j // 2)) % 4
            table_sum(mode, step, (pos + shift) % 4)

            @pl.when(j == 0)
            def _():
                part[mode, step, 0] = fsum[...].astype(BF16)
                leaf_copy(mode, step, 0).start()
                leaf_copy(mode, step, 1).start()

            @pl.when(j == 1)
            def _():
                own[mode, step] = fsum[...]

            @pl.when(j >= 2)
            def _():
                side = j - 2
                leaf_copy(mode, step, side).wait_recv()
                at_row = pl.multiple_of(side * HALF, HALF)
                fsum[pl.ds(at_row, HALF), :] += leaf[mode, step, side].astype(F32)
                part[mode, step, 1 + side] = fsum[...].astype(BF16)
                near_copy(mode, step, side).start()

            return c

        lax.fori_loop(0, 8, table, 0)

        @pl.when(step > 0)
        def _():
            finish(step - 1)

        return c

    def finish(step):
        def one(mode, c):
            near_copy(mode, step, 0).wait_recv()
            near_copy(mode, step, 1).wait_recv()
            zsend[mode, step] = (own[mode, step] + near[mode, step, 0].astype(F32)
                                 + near[mode, step, 1].astype(F32)).astype(BF16)

            @pl.when(pair_of(step) * 2 + mode - z != 0)
            def _():
                z_copy(mode, step).start()

            return c

        lax.fori_loop(0, 2, one, 0)

    lax.fori_loop(0, STEPS, step_body, 0)
    finish(STEPS - 1)

    fsum[...] = zsend[z % 2, STEPS - 1].astype(F32)

    def gather_z(d, c):
        src = (z + d) % NZ
        z_arrival(src).wait_recv()
        fsum[...] += zrecv[src].astype(F32)
        return c

    lax.fori_loop(1, 8, gather_z, 0)

    total = fsum[...]
    high = total.astype(BF16)
    low = (total - high.astype(F32)).astype(BF16)
    weights = proj_ref[0]
    full = (jnp.dot(high, weights, preferred_element_type=F32)
            + jnp.dot(low, weights, preferred_element_type=F32))
    full = jnp.where(lax.broadcasted_iota(jnp.int32, (ROWS, 128), 1) < widths_ref[tab], full, 0.0)
    fsum[...] = full
    for h in range(32):
        hot_all[pl.ds(h, 1), :] = fsum[pl.ds(hot_ref[0, h], 1), :]
    give = remote(hot_all.at[pl.ds(pl.multiple_of((1 - rep) * 16, 16), 16)], hot_got, hot_s, hot_r, {"rep": 1 - rep})
    give.start()
    is_hot = rows == hot_ref[0, 0]
    for h in range(1, 32):
        is_hot = is_hot | (rows == hot_ref[0, h])
    cold_ref[0, 0] = jnp.where(is_hot, 0.0, full)
    give.wait()
    hotout_ref[0] = hot_all[pl.ds(pl.multiple_of(rep * 16, 16), 16), :] + hot_got[...]

    def drain(i, c):
        mode = i % 2
        step = i // 2
        for d in range(1, 4):
            raw_copy(mode, step, d).wait_send()
        for side in range(2):
            leaf_copy(mode, step, side).wait_send()
            near_copy(mode, step, side).wait_send()

        @pl.when(pair_of(step) * 2 + mode - z != 0)
        def _():
            z_copy(mode, step).wait_send()

        return c

    lax.fori_loop(0, 8, drain, 0)


def shards(grad_out, indices, projections, widths, hot_ids):
    z = (lax.axis_index("tab") // NX) % NZ
    by_place = indices.reshape(NY, NZ, NX, 2, 128)
    y_first = by_place.transpose(1, 2, 0, 3, 4).reshape(NZ, 4, 8, 128)
    x_first = by_place.transpose(1, 0, 2, 3, 4).reshape(NZ, 4, 8, 128)
    idx = jnp.where(z % 2 == 0, y_first, x_first)
    vmem = pl.BlockSpec(memory_space=pltpu.VMEM)
    smem = pl.BlockSpec(memory_space=pltpu.SMEM)
    dma = pltpu.SemaphoreType.DMA
    cold, hot = pl.pallas_call(
        kernel,
        out_shape=(jax.ShapeDtypeStruct((1, 1, ROWS, 128), F32), jax.ShapeDtypeStruct((1, 16, 128), F32)),
        in_specs=[pl.BlockSpec(memory_space=pl.ANY), vmem, vmem, smem, smem],
        out_specs=(vmem, vmem),
        scratch_shapes=[
            pltpu.VMEM((4, 4, 256, 8, 128), BF16),
            pltpu.VMEM((2048, 128), F32),
            pltpu.VMEM((2, 4, 4, 4, 256, 128), BF16),
            pltpu.VMEM((2, 4, 3, 4, 256, 128), BF16),
            pltpu.VMEM((ROWS, 128), F32),
            pltpu.VMEM((2, 4, ROWS, 128), F32),
            pltpu.VMEM((2, 4, 3, ROWS, 128), BF16),
            pltpu.VMEM((2, 4, 2, ROWS // 2, 128), BF16),
            pltpu.VMEM((2, 4, 2, ROWS, 128), BF16),
            pltpu.VMEM((2, 4, ROWS, 128), BF16),
            pltpu.VMEM((8, ROWS, 128), BF16),
            pltpu.VMEM((2, 4, 4, 8, 128), jnp.int32),
            pltpu.VMEM((2, 4, 4, 8, 128), jnp.int32),
            pltpu.VMEM((32, 128), F32),
            pltpu.VMEM((16, 128), F32),
            dma((4, 4)), dma((2, 4, 3)), dma((2, 4, 3)), dma((2, 4, 2)), dma((2, 4, 2)),
            dma((2, 4, 2)), dma((2, 4, 2)), dma((2, 4)), dma((8,)),
            dma((7,)), dma((7,)), dma((2, 3)), dma((2, 3)), dma, dma,
        ],
        compiler_params=pltpu.CompilerParams(
            collective_id=0, has_side_effects=True, vmem_limit_bytes=64_000_000),
    )(grad_out, idx, projections, widths, hot_ids)
    return cold, hot


def solution(mesh):
    placed = (
        P(("rep", "tab"), None, None),
        P("tab", "rep"),
        P("tab", None, None),
        P(),
        P("tab", None),
    )
    return jax.shard_map(
        shards,
        mesh=mesh,
        in_specs=placed,
        out_specs=(P("rep", "tab", None, None), P("tab", "rep", None)),
        check_vma=False,
    )
```

```python
import jax
import jax.numpy as jnp
from jax import lax
from jax.experimental import pallas as pl
from jax.experimental.pallas import tpu as pltpu
from jax.sharding import PartitionSpec as P

ROWS = 1024
NX, NY, NZ = 4, 4, 8
STEPS = 4
F32 = jnp.float32
BF16 = jnp.bfloat16


def kernel(grad_ref, idx_ref, proj_ref, widths_ref, hot_ref, cold_ref, hotout_ref,
           stage, tmp, turn, raw, fsum, own, joined, part, leaf, near, zsend, zrecv,
           zi, pi, hot_all, hot_got,
           load_sem, raw_s, raw_r, leaf_s, leaf_r, near_s, near_r, z_s, z_r,
           iz_s, iz_r, iq_s, iq_r, hot_s, hot_r):
    rep = lax.axis_index("rep")
    tab = lax.axis_index("tab")
    x = tab % NX
    z = (tab // NX) % NZ
    y = tab // (NX * NZ)

    def at(px, py, pz):
        return {"tab": (py * NZ + pz) * NX + px}

    def peer(mode, along, shift):
        on_y = (1 - along) * (1 - mode) + along * mode
        return at((x + (1 - on_y) * shift) % NX, (y + on_y * shift) % NY, z)

    def remote(src, dst, s, r, dev):
        return pltpu.make_async_remote_copy(
            src_ref=src, dst_ref=dst, send_sem=s, recv_sem=r,
            device_id=dev, device_id_type=pl.DeviceIdType.MESH)

    def home_of(mode):
        return (z + mode + 1) % 2

    def offset_of(mode, step):
        home = 4 - 2 * step + (step // 2) * (6 + 4 * (step % 2))
        return home_of(mode) * home + (1 - home_of(mode)) * (7 - home)

    def pair_of(mode, step):
        return ((z + offset_of(mode, step) + 8) % NZ) // 2

    def nth_pair(n):
        return (z // 2 + 2 + 3 * n + 3 * (n // 2) + 2 * (n // 3) + 4) % 4

    def load(n, d):
        tile = ((y + d) % NY) * 4 + nth_pair(n)
        return pltpu.make_async_copy(
            grad_ref.at[:, pl.ds(pl.multiple_of(tile * 8, 8), 8), :],
            stage.at[n, d], load_sem.at[n, d])

    def start_loads(i, c):
        load(i // 4, i % 4).start()
        return c

    lax.fori_loop(0, 16, start_loads, 0)

    barrier = pltpu.get_barrier_semaphore()

    def greet(dev):
        pl.semaphore_signal(barrier, inc=1, device_id=dev, device_id_type=pl.DeviceIdType.MESH)

    for d in range(1, 4):
        greet(at((x + d) % NX, y, z))
        greet(at(x, (y + d) % NY, z))
    for d in range(1, 8):
        greet(at(x, y, (z + d) % NZ))
    greet({"rep": 1 - rep})
    pl.semaphore_wait(barrier, 14)

    def iz(d):
        to = (z + d) % NZ
        return remote(idx_ref.at[to], zi.at[z % 2, z // 2], iz_s.at[d - 1], iz_r.at[d - 1], at(x, y, to))

    for d in range(1, 8):
        iz(d).start()
    zi[z % 2, z // 2] = idx_ref[z]

    def raw_copy(mode, step, d):
        pos = y * (1 - mode) + x * mode
        return remote(turn.at[mode, pair_of(mode, step), (pos + d) % 4], raw.at[mode, step, d - 1],
                      raw_s.at[mode, step, d - 1], raw_r.at[mode, step, d - 1], peer(mode, 0, d))

    def relayout(i, c):
        n = i // 4
        d = i % 4
        load(n, d).wait()
        tmp[...] = stage[n, d].astype(F32).reshape(2048, 128)
        to_y = (y + d) % NY
        pair = nth_pair(n)
        for px in range(4):
            turn[0, pair, to_y, px] = tmp[pl.ds(px, 256, stride=8), :].astype(BF16)
        for px in range(4):
            turn[1, pair, px, to_y] = tmp[pl.ds(4 + px, 256, stride=8), :].astype(BF16)
        return c

    def send_raw(step):
        def send(i, c):
            raw_copy(i % 2, step, i // 2 + 1).start()
            return c

        lax.fori_loop(0, 6, send, 0)

    lax.fori_loop(0, 8, relayout, 0)
    send_raw(0)
    lax.fori_loop(8, 16, relayout, 0)
    send_raw(1)

    def iq(mode, d):
        pos = x * (1 - mode) + y * mode
        return remote(zi.at[mode, :, (pos + d) % 4], pi.at[mode, :, pos],
                      iq_s.at[mode, d - 1], iq_r.at[mode, d - 1], peer(mode, 1, d))

    for d in range(1, 8):
        iz(d).wait()
    for mode in range(2):
        for d in range(1, 4):
            iq(mode, d).start()
    pi[0, :, x] = zi[0, :, x]
    pi[1, :, y] = zi[1, :, y]
    for mode in range(2):
        for d in range(1, 4):
            iq(mode, d).wait()

    rows = lax.broadcasted_iota(jnp.int32, (ROWS, 128), 0)

    def onehot(ids, src):
        halves = []
        for h in range(2):
            line = pi[ids + (pl.ds(2 * src + h, 1), slice(None))]
            halves.append(jnp.where(rows == line, F32(1), F32(0)).astype(BF16))
        return jnp.concatenate(halves, axis=1)

    def table_sum(mode, step, dest):
        pos = y * (1 - mode) + x * mode
        pair = pair_of(mode, step)
        values = jnp.concatenate([turn[mode, pair, pos, dest]] + [raw[mode, step, d - 1, dest] for d in range(1, 4)], axis=0)
        ones = jnp.concatenate([onehot((mode, pair, dest), (pos + 4 - d) % 4) for d in range(4)], axis=1)
        fsum[...] = jnp.dot(ones, values, preferred_element_type=F32)

    HALF = ROWS // 2

    def half(h):
        return pl.ds(pl.multiple_of(h * HALF, HALF), HALF)

    def leaf_copy(mode, step, side):
        return remote(part.at[mode, step, 0, half(side)], leaf.at[mode, step, side],
                      leaf_s.at[mode, step, side], leaf_r.at[mode, step, side], peer(mode, 1, 1 + 2 * side))

    def near_copy(mode, step, side, h):
        return remote(part.at[mode, step, 1 + side, half(h)], near.at[mode, step, side, half(h)],
                      near_s.at[mode, step, side, h], near_r.at[mode, step, side, h], peer(mode, 1, 1 + 2 * side))

    def z_copy(mode, step, h):
        to = (z + 1 + 6 * ((home_of(mode) + step) % 2)) % NZ
        return remote(zsend.at[mode, step, half(h)], zrecv.at[mode, step, half(h)],
                      z_s.at[mode, step, h], z_r.at[mode, step, h], at(x, y, to))

    def step_body(step, c):
        def arrive(i, c):
            raw_copy(i % 2, step, i // 2 + 1).wait_recv()
            return c

        lax.fori_loop(0, 6, arrive, 0)

        def table(i, c):
            mode = i % 2
            j = i // 2
            pos = x * (1 - mode) + y * mode
            shift = (2 + 3 * j + (j // 2) * (3 - 2 * (j % 2))) % 4
            table_sum(mode, step, (pos + shift) % 4)

            @pl.when(j == 0)
            def _():
                part[mode, step, 0] = fsum[...].astype(BF16)
                leaf_copy(mode, step, 0).start()
                leaf_copy(mode, step, 1).start()

            @pl.when((i == 1) & (step < STEPS - 2))
            def _():
                send_raw(step + 2)

            @pl.when((j == 1) | (j == 2))
            def _():
                side = j - 1
                free = half(1 - side)
                part[mode, step, 1 + side, free] = fsum[free, :].astype(BF16)
                near_copy(mode, step, side, 1 - side).start()
                joined[mode, side] = fsum[half(side), :]

            @pl.when(j == 3)
            def _():
                own[mode, step % 2] = fsum[...]

            return c

        lax.fori_loop(0, 8, table, 0)

        def join(i, c):
            mode = i % 2
            side = i // 2
            leaf_copy(mode, step, side).wait_recv()
            part[mode, step, 1 + side, half(side)] = (joined[mode, side] + leaf[mode, step, side].astype(F32)).astype(BF16)
            near_copy(mode, step, side, side).start()
            return c

        lax.fori_loop(0, 4, join, 0)

        @pl.when(step > 0)
        def _():
            finish(step - 1)

        return c

    def finish(step):
        def one(i, c):
            mode = (1 + z + i) % 2
            h = i // 2
            rows_h = half(h)
            near_copy(mode, step, 0, h).wait_recv()
            near_copy(mode, step, 1, h).wait_recv()
            fsum[rows_h, :] = (own[mode, step % 2, rows_h, :] + near[mode, step, 0, rows_h, :].astype(F32)
                               + near[mode, step, 1, rows_h, :].astype(F32))

            @pl.when(step > 0)
            def _():
                z_copy(mode, step - 1, h).wait_recv()
                fsum[rows_h, :] += zrecv[mode, step - 1, rows_h, :].astype(F32)

            @pl.when((home_of(mode) == 0) | (step < STEPS - 1))
            def _():
                zsend[mode, step, rows_h, :] = fsum[rows_h, :].astype(BF16)
                z_copy(mode, step, h).start()

            return c

        lax.fori_loop(0, 4, one, 0)

    lax.fori_loop(0, STEPS, step_body, 0)
    finish(STEPS - 1)

    for h in range(2):
        z_copy(z % 2, STEPS - 1, h).wait_recv()
        fsum[half(h), :] += zrecv[z % 2, STEPS - 1, half(h), :].astype(F32)

    total = fsum[...]
    high = total.astype(BF16)
    low = (total - high.astype(F32)).astype(BF16)
    weights = proj_ref[0]
    full = (jnp.dot(high, weights, preferred_element_type=F32)
            + jnp.dot(low, weights, preferred_element_type=F32))
    full = jnp.where(lax.broadcasted_iota(jnp.int32, (ROWS, 128), 1) < widths_ref[tab], full, 0.0)
    fsum[...] = full
    for h in range(32):
        hot_all[pl.ds(h, 1), :] = fsum[pl.ds(hot_ref[0, h], 1), :]
    give = remote(hot_all.at[pl.ds(pl.multiple_of((1 - rep) * 16, 16), 16)], hot_got, hot_s, hot_r, {"rep": 1 - rep})
    give.start()
    is_hot = rows == hot_ref[0, 0]
    for h in range(1, 32):
        is_hot = is_hot | (rows == hot_ref[0, h])
    cold_ref[0, 0] = jnp.where(is_hot, 0.0, full)
    give.wait()
    hotout_ref[0] = hot_all[pl.ds(pl.multiple_of(rep * 16, 16), 16), :] + hot_got[...]

    def drain(i, c):
        mode = i % 2
        step = i // 2
        for d in range(1, 4):
            raw_copy(mode, step, d).wait_send()
        for side in range(2):
            leaf_copy(mode, step, side).wait_send()
            for h in range(2):
                near_copy(mode, step, side, h).wait_send()

        @pl.when((home_of(mode) == 0) | (step < STEPS - 1))
        def _():
            for h in range(2):
                z_copy(mode, step, h).wait_send()

        return c

    lax.fori_loop(0, 8, drain, 0)


def shards(grad_out, indices, projections, widths, hot_ids):
    z = (lax.axis_index("tab") // NX) % NZ
    by_place = indices.reshape(NY, NZ, NX, 2, 128)
    y_first = by_place.transpose(1, 2, 0, 3, 4).reshape(NZ, 4, 8, 128)
    x_first = by_place.transpose(1, 0, 2, 3, 4).reshape(NZ, 4, 8, 128)
    idx = jnp.where(z % 2 == 0, y_first, x_first)
    vmem = pl.BlockSpec(memory_space=pltpu.VMEM)
    smem = pl.BlockSpec(memory_space=pltpu.SMEM)
    dma = pltpu.SemaphoreType.DMA
    cold, hot = pl.pallas_call(
        kernel,
        out_shape=(jax.ShapeDtypeStruct((1, 1, ROWS, 128), F32), jax.ShapeDtypeStruct((1, 16, 128), F32)),
        in_specs=[pl.BlockSpec(memory_space=pl.ANY), vmem, vmem, smem, smem],
        out_specs=(vmem, vmem),
        scratch_shapes=[
            pltpu.VMEM((4, 4, 256, 8, 128), BF16),
            pltpu.VMEM((2048, 128), F32),
            pltpu.VMEM((2, 4, 4, 4, 256, 128), BF16),
            pltpu.VMEM((2, 4, 3, 4, 256, 128), BF16),
            pltpu.VMEM((ROWS, 128), F32),
            pltpu.VMEM((2, 2, ROWS, 128), F32),
            pltpu.VMEM((2, 2, ROWS // 2, 128), F32),
            pltpu.VMEM((2, 4, 3, ROWS, 128), BF16),
            pltpu.VMEM((2, 4, 2, ROWS // 2, 128), BF16),
            pltpu.VMEM((2, 4, 2, ROWS, 128), BF16),
            pltpu.VMEM((2, 4, ROWS, 128), BF16),
            pltpu.VMEM((2, 4, ROWS, 128), BF16),
            pltpu.VMEM((2, 4, 4, 8, 128), jnp.int32),
            pltpu.VMEM((2, 4, 4, 8, 128), jnp.int32),
            pltpu.VMEM((32, 128), F32),
            pltpu.VMEM((16, 128), F32),
            dma((4, 4)), dma((2, 4, 3)), dma((2, 4, 3)), dma((2, 4, 2)), dma((2, 4, 2)),
            dma((2, 4, 2, 2)), dma((2, 4, 2, 2)), dma((2, 4, 2)), dma((2, 4, 2)),
            dma((7,)), dma((7,)), dma((2, 3)), dma((2, 3)), dma, dma,
        ],
        compiler_params=pltpu.CompilerParams(
            collective_id=0, has_side_effects=True, vmem_limit_bytes=64_000_000),
    )(grad_out, idx, projections, widths, hot_ids)
    return cold, hot


def solution(mesh):
    placed = (
        P(("rep", "tab"), None, None),
        P("tab", "rep"),
        P("tab", None, None),
        P(),
        P("tab", None),
    )
    return jax.shard_map(
        shards,
        mesh=mesh,
        in_specs=placed,
        out_specs=(P("rep", "tab", None, None), P("tab", "rep", None)),
        check_vma=False,
    )
```

```python
import jax
import jax.numpy as jnp
from jax import lax
from jax.experimental import pallas as pl
from jax.experimental.pallas import tpu as pltpu
from jax.sharding import PartitionSpec as P

ROWS = 1024
NX, NY, NZ = 4, 4, 8
STEPS = 4
F32 = jnp.float32
BF16 = jnp.bfloat16


def kernel(grad_ref, idx_ref, hot_ref, sums_ref, hotsum_ref,
           stage, tmp, turn, raw, fsum, own, joined, part, leaf, near, zsend, zrecv,
           zi, pi, hot_all, hot_got,
           load_sem, raw_s, raw_r, leaf_s, leaf_r, near_s, near_r, z_s, z_r,
           iz_s, iz_r, iq_s, iq_r, hot_s, hot_r, own_sem, round_a, round_b):
    rep = lax.axis_index("rep")
    tab = lax.axis_index("tab")
    x = tab % NX
    z = (tab // NX) % NZ
    y = tab // (NX * NZ)

    def at(px, py, pz):
        return {"tab": (py * NZ + pz) * NX + px}

    def peer(mode, along, shift):
        on_y = (1 - along) * (1 - mode) + along * mode
        return at((x + (1 - on_y) * shift) % NX, (y + on_y * shift) % NY, z)

    def remote(src, dst, s, r, dev):
        return pltpu.make_async_remote_copy(
            src_ref=src, dst_ref=dst, send_sem=s, recv_sem=r,
            device_id=dev, device_id_type=pl.DeviceIdType.MESH)

    def home_of(mode):
        return (z + mode + 1) % 2

    def offset_of(mode, step):
        home = 4 - 2 * step + (step // 2) * (6 + 4 * (step % 2))
        return home_of(mode) * home + (1 - home_of(mode)) * (7 - home)

    def pair_of(mode, step):
        return ((z + offset_of(mode, step) + 8) % NZ) // 2

    def nth_pair(n):
        return (z // 2 + 2 + 3 * n + 3 * (n // 2) + 2 * (n // 3) + 4) % 4

    def load(n, d):
        tile = ((y + d) % NY) * 4 + nth_pair(n)
        return pltpu.make_async_copy(
            grad_ref.at[:, pl.ds(pl.multiple_of(tile * 8, 8), 8), :],
            stage.at[n, d], load_sem.at[n, d])

    def start_loads(i, c):
        load(i // 4, i % 4).start()
        return c

    lax.fori_loop(0, 16, start_loads, 0)

    barrier = pltpu.get_barrier_semaphore()

    def greet(dev):
        pl.semaphore_signal(barrier, inc=1, device_id=dev, device_id_type=pl.DeviceIdType.MESH)

    for d in range(1, 4):
        greet(at((x + d) % NX, y, z))
        greet(at(x, (y + d) % NY, z))
    for d in (1, 7):
        greet(at(x, y, (z + d) % NZ))
    greet({"rep": 1 - rep})
    pl.semaphore_wait(barrier, 9)

    def raw_copy(mode, step, d):
        pos = y * (1 - mode) + x * mode
        return remote(turn.at[mode, pair_of(mode, step), (pos + d) % 4], raw.at[mode, step, d - 1],
                      raw_s.at[mode, step, d - 1], raw_r.at[mode, step, d - 1], peer(mode, 0, d))

    def relayout(i, c):
        n = i // 4
        d = i % 4
        load(n, d).wait()
        tmp[...] = stage[n, d].astype(F32).reshape(2048, 128)
        to_y = (y + d) % NY
        pair = nth_pair(n)
        for px in range(4):
            turn[0, pair, to_y, px] = tmp[pl.ds(px, 256, stride=8), :].astype(BF16)
        for px in range(4):
            turn[1, pair, px, to_y] = tmp[pl.ds(4 + px, 256, stride=8), :].astype(BF16)
        return c

    def send_raw(step):
        def send(i, c):
            raw_copy(i % 2, step, i // 2 + 1).start()
            return c

        lax.fori_loop(0, 6, send, 0)

    lax.fori_loop(0, 8, relayout, 0)
    send_raw(0)

    for sem, away in ((round_a, 1), (round_b, 2)):
        for d in (away, 8 - away):
            pl.semaphore_signal(sem, inc=1, device_id=at(x, y, (z + d) % NZ), device_id_type=pl.DeviceIdType.MESH)
        pl.semaphore_wait(sem, 2)

    def iz(d):
        to = (z + d) % NZ
        return remote(idx_ref.at[:, to], zi.at[z % 2, z // 2], iz_s.at[d - 1], iz_r.at[d - 1], at(x, y, to))

    for d in range(1, 8):
        iz(d).start()
    own_idx = pltpu.make_async_copy(idx_ref.at[:, z], zi.at[z % 2, z // 2], own_sem)
    own_idx.start()
    lax.fori_loop(8, 16, relayout, 0)
    own_idx.wait()

    def iq(mode, d):
        pos = x * (1 - mode) + y * mode
        to = (pos + d) % 4
        return remote(zi.at[0, :, :, to] if mode == 0 else zi.at[1, :, to], pi.at[mode, :, pos],
                      iq_s.at[mode, d - 1], iq_r.at[mode, d - 1], peer(mode, 1, d))

    for d in range(1, 8):
        iz(d).wait()
    for mode in range(2):
        for d in range(1, 4):
            iq(mode, d).start()
    send_raw(1)
    pi[0, :, x] = zi[0, :, :, x]
    pi[1, :, y] = zi[1, :, y]
    for mode in range(2):
        for d in range(1, 4):
            iq(mode, d).wait()

    rows = lax.broadcasted_iota(jnp.int32, (ROWS, 128), 0)

    def onehot(ids, src):
        halves = []
        for h in range(2):
            line = pi[ids + (src, pl.ds(h, 1), slice(None))]
            halves.append(jnp.where(rows == line, F32(1), F32(0)).astype(BF16))
        return jnp.concatenate(halves, axis=1)

    def table_sum(mode, step, dest):
        pos = y * (1 - mode) + x * mode
        pair = pair_of(mode, step)
        values = jnp.concatenate([turn[mode, pair, pos, dest]] + [raw[mode, step, d - 1, dest] for d in range(1, 4)], axis=0)
        ones = jnp.concatenate([onehot((mode, pair, dest), (pos + 4 - d) % 4) for d in range(4)], axis=1)
        fsum[...] = jnp.dot(ones, values, preferred_element_type=F32)

    HALF = ROWS // 2

    def half(h):
        return pl.ds(pl.multiple_of(h * HALF, HALF), HALF)

    def leaf_copy(mode, step, side):
        return remote(part.at[mode, step, 0, half(side)], leaf.at[mode, step, side],
                      leaf_s.at[mode, step, side], leaf_r.at[mode, step, side], peer(mode, 1, 1 + 2 * side))

    def near_copy(mode, step, side, h):
        return remote(part.at[mode, step, 1 + side, half(h)], near.at[mode, step, side, half(h)],
                      near_s.at[mode, step, side, h], near_r.at[mode, step, side, h], peer(mode, 1, 1 + 2 * side))

    def z_copy(mode, step, h):
        to = (z + 1 + 6 * ((home_of(mode) + step) % 2)) % NZ
        return remote(zsend.at[mode, step, half(h)], zrecv.at[mode, step, half(h)],
                      z_s.at[mode, step, h], z_r.at[mode, step, h], at(x, y, to))

    def step_body(step, c):
        def arrive(i, c):
            raw_copy(i % 2, step, i // 2 + 1).wait_recv()
            return c

        lax.fori_loop(0, 6, arrive, 0)

        def table(i, c):
            mode = i % 2
            j = i // 2
            pos = x * (1 - mode) + y * mode
            shift = (2 + 3 * j + (j // 2) * (3 - 2 * (j % 2))) % 4
            table_sum(mode, step, (pos + shift) % 4)

            @pl.when(j == 0)
            def _():
                part[mode, step, 0] = fsum[...].astype(BF16)
                leaf_copy(mode, step, 0).start()
                leaf_copy(mode, step, 1).start()

            @pl.when((i == 1) & (step < STEPS - 2))
            def _():
                send_raw(step + 2)

            @pl.when((j == 1) | (j == 2))
            def _():
                side = j - 1
                free = half(1 - side)
                part[mode, step, 1 + side, free] = fsum[free, :].astype(BF16)
                near_copy(mode, step, side, 1 - side).start()
                joined[mode, side] = fsum[half(side), :]

            @pl.when(j == 3)
            def _():
                own[mode, step % 2] = fsum[...]

            return c

        lax.fori_loop(0, 8, table, 0)

        def join(i, c):
            mode = i % 2
            side = i // 2
            leaf_copy(mode, step, side).wait_recv()
            part[mode, step, 1 + side, half(side)] = (joined[mode, side] + leaf[mode, step, side].astype(F32)).astype(BF16)
            near_copy(mode, step, side, side).start()
            return c

        lax.fori_loop(0, 4, join, 0)

        @pl.when(step > 0)
        def _():
            finish(step - 1)

        return c

    def finish(step):
        def one(i, c):
            mode = (1 + z + i) % 2
            h = i // 2
            rows_h = half(h)
            near_copy(mode, step, 0, h).wait_recv()
            near_copy(mode, step, 1, h).wait_recv()
            fsum[rows_h, :] = (own[mode, step % 2, rows_h, :] + near[mode, step, 0, rows_h, :].astype(F32)
                               + near[mode, step, 1, rows_h, :].astype(F32))

            @pl.when(step > 0)
            def _():
                z_copy(mode, step - 1, h).wait_recv()
                fsum[rows_h, :] += zrecv[mode, step - 1, rows_h, :].astype(F32)

            @pl.when((home_of(mode) == 0) | (step < STEPS - 1))
            def _():
                zsend[mode, step, rows_h, :] = fsum[rows_h, :].astype(BF16)
                z_copy(mode, step, h).start()

            return c

        lax.fori_loop(0, 4, one, 0)

    lax.fori_loop(0, STEPS, step_body, 0)
    finish(STEPS - 1)

    for h in range(2):
        z_copy(z % 2, STEPS - 1, h).wait_recv()
        sums_ref[half(h), :] = fsum[half(h), :] + zrecv[z % 2, STEPS - 1, half(h), :].astype(F32)

    for h in range(32):
        hot_all[pl.ds(h, 1), :] = sums_ref[pl.ds(hot_ref[0, h], 1), :]
    give = remote(hot_all.at[pl.ds(pl.multiple_of((1 - rep) * 16, 16), 16)], hot_got, hot_s, hot_r, {"rep": 1 - rep})
    give.start()

    def drain(i, c):
        mode = i % 2
        step = i // 2
        for d in range(1, 4):
            raw_copy(mode, step, d).wait_send()
        for side in range(2):
            leaf_copy(mode, step, side).wait_send()
            for h in range(2):
                near_copy(mode, step, side, h).wait_send()

        @pl.when((home_of(mode) == 0) | (step < STEPS - 1))
        def _():
            for h in range(2):
                z_copy(mode, step, h).wait_send()

        return c

    lax.fori_loop(0, 8, drain, 0)
    give.wait()
    hotsum_ref[...] = hot_all[pl.ds(pl.multiple_of(rep * 16, 16), 16), :] + hot_got[...]


def outputs(sums_ref, hotsum_ref, proj_ref, widths_ref, hot_ref, cold_ref, hotout_ref):
    width = widths_ref[lax.axis_index("tab")]
    weights = proj_ref[0]

    def project(total):
        high = total.astype(BF16)
        low = (total - high.astype(F32)).astype(BF16)
        full = (jnp.dot(high, weights, preferred_element_type=F32)
                + jnp.dot(low, weights, preferred_element_type=F32))
        return jnp.where(lax.broadcasted_iota(jnp.int32, full.shape, 1) < width, full, 0.0)

    rows = lax.broadcasted_iota(jnp.int32, (ROWS, 128), 0)
    is_hot = rows == hot_ref[0, 0]
    for h in range(1, 32):
        is_hot = is_hot | (rows == hot_ref[0, h])
    cold_ref[0, 0] = jnp.where(is_hot, 0.0, project(sums_ref[...]))
    hotout_ref[0] = project(hotsum_ref[...])


def shards(grad_out, indices, projections, widths, hot_ids):
    idx = indices.reshape(NY, NZ, NX, 2, 128)
    vmem = pl.BlockSpec(memory_space=pltpu.VMEM)
    smem = pl.BlockSpec(memory_space=pltpu.SMEM)
    dma = pltpu.SemaphoreType.DMA
    sums, hot_sums = pl.pallas_call(
        kernel,
        out_shape=(jax.ShapeDtypeStruct((ROWS, 128), F32), jax.ShapeDtypeStruct((16, 128), F32)),
        in_specs=[pl.BlockSpec(memory_space=pl.ANY), pl.BlockSpec(memory_space=pl.ANY), smem],
        out_specs=(vmem, vmem),
        scratch_shapes=[
            pltpu.VMEM((4, 4, 256, 8, 128), BF16),
            pltpu.VMEM((2048, 128), F32),
            pltpu.VMEM((2, 4, 4, 4, 256, 128), BF16),
            pltpu.VMEM((2, 4, 3, 4, 256, 128), BF16),
            pltpu.VMEM((ROWS, 128), F32),
            pltpu.VMEM((2, 2, ROWS, 128), F32),
            pltpu.VMEM((2, 2, ROWS // 2, 128), F32),
            pltpu.VMEM((2, 4, 3, ROWS, 128), BF16),
            pltpu.VMEM((2, 4, 2, ROWS // 2, 128), BF16),
            pltpu.VMEM((2, 4, 2, ROWS, 128), BF16),
            pltpu.VMEM((2, 4, ROWS, 128), BF16),
            pltpu.VMEM((2, 4, ROWS, 128), BF16),
            pltpu.VMEM((2, 4, 4, 4, 2, 128), jnp.int32),
            pltpu.VMEM((2, 4, 4, 4, 2, 128), jnp.int32),
            pltpu.VMEM((32, 128), F32),
            pltpu.VMEM((16, 128), F32),
            dma((4, 4)), dma((2, 4, 3)), dma((2, 4, 3)), dma((2, 4, 2)), dma((2, 4, 2)),
            dma((2, 4, 2, 2)), dma((2, 4, 2, 2)), dma((2, 4, 2)), dma((2, 4, 2)),
            dma((7,)), dma((7,)), dma((2, 3)), dma((2, 3)), dma, dma, dma,
            pltpu.SemaphoreType.REGULAR, pltpu.SemaphoreType.REGULAR,
        ],
        compiler_params=pltpu.CompilerParams(
            collective_id=0, has_side_effects=True, vmem_limit_bytes=64_000_000),
    )(grad_out, idx, hot_ids)
    return pl.pallas_call(
        outputs,
        out_shape=(jax.ShapeDtypeStruct((1, 1, ROWS, 128), F32), jax.ShapeDtypeStruct((1, 16, 128), F32)),
        in_specs=[vmem, vmem, vmem, smem, smem],
        out_specs=(vmem, vmem),
    )(sums, hot_sums, projections, widths, hot_ids)


def solution(mesh):
    placed = (
        P(("rep", "tab"), None, None),
        P("tab", "rep"),
        P("tab", None, None),
        P(),
        P("tab", None),
    )
    return jax.shard_map(
        shards,
        mesh=mesh,
        in_specs=placed,
        out_specs=(P("rep", "tab", None, None), P("tab", "rep", None)),
        check_vma=False,
    )
```

```python
import jax
import jax.numpy as jnp
from jax import lax
from jax.experimental import pallas as pl
from jax.experimental.pallas import tpu as pltpu
from jax.sharding import PartitionSpec as P

ROWS = 1024
NX, NY, NZ = 4, 4, 8
STEPS = 4
PRE = 1
F32 = jnp.float32
BF16 = jnp.bfloat16


def kernel(grad_ref, idx_ref, hot_ref, sums_ref, hotsum_ref,
           stage, tmp, turn, raw, fsum, own, joined, part, leaf, near, zsend, zrecv, early, before,
           zi, pi, hot_all, hot_got,
           load_sem, raw_s, raw_r, leaf_s, leaf_r, near_s, near_r, z_s, z_r, early_s, early_r,
           iz_s, iz_r, iq_s, iq_r, hot_s, hot_r, own_sem, round_a, round_b):
    rep = lax.axis_index("rep")
    tab = lax.axis_index("tab")
    x = tab % NX
    z = (tab // NX) % NZ
    y = tab // (NX * NZ)

    def at(px, py, pz):
        return {"tab": (py * NZ + pz) * NX + px}

    def peer(mode, along, shift):
        on_y = (1 - along) * (1 - mode) + along * mode
        return at((x + (1 - on_y) * shift) % NX, (y + on_y * shift) % NY, z)

    def remote(src, dst, s, r, dev):
        return pltpu.make_async_remote_copy(
            src_ref=src, dst_ref=dst, send_sem=s, recv_sem=r,
            device_id=dev, device_id_type=pl.DeviceIdType.MESH)

    def home_of(mode):
        return (z + mode + 1) % 2

    def offset_of(mode, step):
        home = 4 - 2 * step + (step // 2) * (6 + 4 * (step % 2))
        return home_of(mode) * home + (1 - home_of(mode)) * (7 - home)

    def pair_of(mode, step):
        return ((z + offset_of(mode, step) + 8) % NZ) // 2

    def nth_pair(n):
        return (z // 2 + 2 + 3 * n + 3 * (n // 2) + 2 * (n // 3) + 4) % 4

    def load(n, d):
        tile = ((y + d) % NY) * 4 + nth_pair(n)
        return pltpu.make_async_copy(
            grad_ref.at[:, pl.ds(pl.multiple_of(tile * 8, 8), 8), :],
            stage.at[n, d], load_sem.at[n, d])

    def start_loads(i, c):
        load(i // 4, i % 4).start()
        return c

    lax.fori_loop(0, 16, start_loads, 0)

    barrier = pltpu.get_barrier_semaphore()

    def greet(dev):
        pl.semaphore_signal(barrier, inc=1, device_id=dev, device_id_type=pl.DeviceIdType.MESH)

    for d in range(1, 4):
        greet(at((x + d) % NX, y, z))
        greet(at(x, (y + d) % NY, z))
    for d in (1, 7):
        greet(at(x, y, (z + d) % NZ))
    greet({"rep": 1 - rep})
    pl.semaphore_wait(barrier, 9)

    def raw_copy(mode, step, d):
        pos = y * (1 - mode) + x * mode
        return remote(turn.at[mode, pair_of(mode, step), (pos + d) % 4], raw.at[mode, step, d - 1],
                      raw_s.at[mode, step, d - 1], raw_r.at[mode, step, d - 1], peer(mode, 0, d))

    def relayout(i, c):
        n = i // 4
        d = i % 4
        load(n, d).wait()
        tmp[...] = stage[n, d].astype(F32).reshape(2048, 128)
        to_y = (y + d) % NY
        pair = nth_pair(n)
        for px in range(4):
            turn[0, pair, to_y, px] = tmp[pl.ds(px, 256, stride=8), :].astype(BF16)
        for px in range(4):
            turn[1, pair, px, to_y] = tmp[pl.ds(4 + px, 256, stride=8), :].astype(BF16)
        return c

    def send_raw(step):
        def send(i, c):
            raw_copy(i % 2, step, i // 2 + 1).start()
            return c

        lax.fori_loop(0, 6, send, 0)

    lax.fori_loop(0, 8, relayout, 0)
    send_raw(0)

    for sem, away in ((round_a, 1), (round_b, 2)):
        for d in (away, 8 - away):
            pl.semaphore_signal(sem, inc=1, device_id=at(x, y, (z + d) % NZ), device_id_type=pl.DeviceIdType.MESH)
        pl.semaphore_wait(sem, 2)

    def iz(d):
        to = (z + d) % NZ
        return remote(idx_ref.at[:, to], zi.at[z % 2, z // 2], iz_s.at[d - 1], iz_r.at[d - 1], at(x, y, to))

    for d in range(1, 8):
        iz(d).start()
    own_idx = pltpu.make_async_copy(idx_ref.at[:, z], zi.at[z % 2, z // 2], own_sem)
    own_idx.start()
    lax.fori_loop(8, 16, relayout, 0)
    own_idx.wait()

    def iq(mode, d):
        pos = x * (1 - mode) + y * mode
        to = (pos + d) % 4
        return remote(zi.at[0, :, :, to] if mode == 0 else zi.at[1, :, to], pi.at[mode, :, pos],
                      iq_s.at[mode, d - 1], iq_r.at[mode, d - 1], peer(mode, 1, d))

    for d in range(1, 8):
        iz(d).wait()
    for mode in range(2):
        for d in range(1, 4):
            iq(mode, d).start()
    send_raw(1)
    pi[0, :, x] = zi[0, :, :, x]
    pi[1, :, y] = zi[1, :, y]
    for mode in range(2):
        for d in range(1, 4):
            iq(mode, d).wait()

    rows = lax.broadcasted_iota(jnp.int32, (ROWS, 128), 0)

    def onehot(ids, src):
        halves = []
        for h in range(2):
            line = pi[ids + (src, pl.ds(h, 1), slice(None))]
            halves.append(jnp.where(rows == line, F32(1), F32(0)).astype(BF16))
        return jnp.concatenate(halves, axis=1)

    def table_sum(mode, step, dest):
        pos = y * (1 - mode) + x * mode
        pair = pair_of(mode, step)
        values = jnp.concatenate([turn[mode, pair, pos, dest]] + [raw[mode, step, d - 1, dest] for d in range(1, 4)], axis=0)
        ones = jnp.concatenate([onehot((mode, pair, dest), (pos + 4 - d) % 4) for d in range(4)], axis=1)
        fsum[...] = jnp.dot(ones, values, preferred_element_type=F32)

    HALF = ROWS // 2

    def half(h):
        return pl.ds(pl.multiple_of(h * HALF, HALF), HALF)

    def leaf_copy(mode, step, side):
        return remote(part.at[mode, step - PRE, 0, half(side)], leaf.at[mode, step - PRE, side],
                      leaf_s.at[mode, step - PRE, side], leaf_r.at[mode, step - PRE, side], peer(mode, 1, 1 + 2 * side))

    def near_copy(mode, step, side, h):
        return remote(part.at[mode, step - PRE, 1 + side, half(h)], near.at[mode, step - PRE, side, half(h)],
                      near_s.at[mode, step - PRE, side, h], near_r.at[mode, step - PRE, side, h], peer(mode, 1, 1 + 2 * side))

    def along_z(mode, step):
        return at(x, y, (z + 1 + 6 * ((home_of(mode) + step) % 2)) % NZ)

    def z_copy(mode, step, h):
        return remote(zsend.at[mode, step - PRE, half(h)], zrecv.at[mode, step - PRE, half(h)],
                      z_s.at[mode, step - PRE, h], z_r.at[mode, step - PRE, h], along_z(mode, step))

    def early_copy(mode, step, dest):
        return remote(early.at[mode, step, dest], before.at[mode, step, dest],
                      early_s.at[mode, step, dest], early_r.at[mode, step, dest], along_z(mode, step))

    def step_body(step, c):
        def arrive(i, c):
            raw_copy(i % 2, step, i // 2 + 1).wait_recv()
            return c

        lax.fori_loop(0, 6, arrive, 0)

        def table(i, c):
            mode = i % 2
            j = i // 2
            pos = x * (1 - mode) + y * mode
            shift = (2 + 3 * j + (j // 2) * (3 - 2 * (j % 2))) % 4
            dest = (pos + shift) % 4
            table_sum(mode, step, dest)

            @pl.when((step >= 1) & (step <= PRE))
            def _():
                early_copy(mode, step - 1, dest).wait_recv()
                fsum[...] += before[mode, step - 1, dest].astype(F32)

            @pl.when(step < PRE)
            def _():
                early[mode, step, dest] = fsum[...].astype(BF16)
                early_copy(mode, step, dest).start()

            @pl.when((j == 0) & (step >= PRE))
            def _():
                part[mode, step - PRE, 0] = fsum[...].astype(BF16)
                leaf_copy(mode, step, 0).start()
                leaf_copy(mode, step, 1).start()

            @pl.when((i == 1) & (step < STEPS - 2))
            def _():
                send_raw(step + 2)

            @pl.when(((j == 1) | (j == 2)) & (step >= PRE))
            def _():
                side = j - 1
                free = half(1 - side)
                part[mode, step - PRE, 1 + side, free] = fsum[free, :].astype(BF16)
                near_copy(mode, step, side, 1 - side).start()
                joined[mode, side] = fsum[half(side), :]

            @pl.when((j == 3) & (step >= PRE))
            def _():
                own[mode, step % 2] = fsum[...]

            return c

        lax.fori_loop(0, 8, table, 0)

        def join(i, c):
            mode = i % 2
            side = i // 2
            leaf_copy(mode, step, side).wait_recv()
            part[mode, step - PRE, 1 + side, half(side)] = (joined[mode, side] + leaf[mode, step - PRE, side].astype(F32)).astype(BF16)
            near_copy(mode, step, side, side).start()
            return c

        @pl.when(step >= PRE)
        def _():
            lax.fori_loop(0, 4, join, 0)

        @pl.when(step > PRE)
        def _():
            finish(step - 1)

        return c

    def finish(step):
        def one(i, c):
            mode = (1 + z + i) % 2
            h = i // 2
            rows_h = half(h)
            near_copy(mode, step, 0, h).wait_recv()
            near_copy(mode, step, 1, h).wait_recv()
            fsum[rows_h, :] = (own[mode, step % 2, rows_h, :] + near[mode, step - PRE, 0, rows_h, :].astype(F32)
                               + near[mode, step - PRE, 1, rows_h, :].astype(F32))

            @pl.when(step > PRE)
            def _():
                z_copy(mode, step - 1, h).wait_recv()
                fsum[rows_h, :] += zrecv[mode, step - 1 - PRE, rows_h, :].astype(F32)

            @pl.when((home_of(mode) == 0) | (step < STEPS - 1))
            def _():
                zsend[mode, step - PRE, rows_h, :] = fsum[rows_h, :].astype(BF16)
                z_copy(mode, step, h).start()

            return c

        lax.fori_loop(0, 4, one, 0)

    lax.fori_loop(0, STEPS, step_body, 0)
    finish(STEPS - 1)

    for h in range(2):
        z_copy(z % 2, STEPS - 1, h).wait_recv()
        sums_ref[half(h), :] = fsum[half(h), :] + zrecv[z % 2, STEPS - 1 - PRE, half(h), :].astype(F32)

    for h in range(32):
        hot_all[pl.ds(h, 1), :] = sums_ref[pl.ds(hot_ref[0, h], 1), :]
    give = remote(hot_all.at[pl.ds(pl.multiple_of((1 - rep) * 16, 16), 16)], hot_got, hot_s, hot_r, {"rep": 1 - rep})
    give.start()

    def drain(i, c):
        mode = i % 2
        step = i // 2
        for d in range(1, 4):
            raw_copy(mode, step, d).wait_send()

        @pl.when(step < PRE)
        def _():
            for dest in range(4):
                early_copy(mode, step, dest).wait_send()

        @pl.when(step >= PRE)
        def _():
            for side in range(2):
                leaf_copy(mode, step, side).wait_send()
                for h in range(2):
                    near_copy(mode, step, side, h).wait_send()

        @pl.when((step >= PRE) & ((home_of(mode) == 0) | (step < STEPS - 1)))
        def _():
            for h in range(2):
                z_copy(mode, step, h).wait_send()

        return c

    lax.fori_loop(0, 8, drain, 0)
    give.wait()
    hotsum_ref[...] = hot_all[pl.ds(pl.multiple_of(rep * 16, 16), 16), :] + hot_got[...]


def outputs(sums_ref, hotsum_ref, proj_ref, widths_ref, hot_ref, cold_ref, hotout_ref):
    width = widths_ref[lax.axis_index("tab")]
    weights = proj_ref[0]

    def project(total):
        high = total.astype(BF16)
        low = (total - high.astype(F32)).astype(BF16)
        full = (jnp.dot(high, weights, preferred_element_type=F32)
                + jnp.dot(low, weights, preferred_element_type=F32))
        return jnp.where(lax.broadcasted_iota(jnp.int32, full.shape, 1) < width, full, 0.0)

    cold_ref[0, 0] = project(sums_ref[...])
    for h in range(32):
        cold_ref[0, 0, pl.ds(hot_ref[0, h], 1), :] = jnp.zeros((1, 128), F32)
    hotout_ref[0] = project(hotsum_ref[...])


def shards(grad_out, indices, projections, widths, hot_ids):
    idx = indices.reshape(NY, NZ, NX, 2, 128)
    vmem = pl.BlockSpec(memory_space=pltpu.VMEM)
    smem = pl.BlockSpec(memory_space=pltpu.SMEM)
    dma = pltpu.SemaphoreType.DMA
    sums, hot_sums = pl.pallas_call(
        kernel,
        out_shape=(jax.ShapeDtypeStruct((ROWS, 128), F32), jax.ShapeDtypeStruct((16, 128), F32)),
        in_specs=[pl.BlockSpec(memory_space=pl.ANY), pl.BlockSpec(memory_space=pl.ANY), smem],
        out_specs=(vmem, vmem),
        scratch_shapes=[
            pltpu.VMEM((4, 4, 256, 8, 128), BF16),
            pltpu.VMEM((2048, 128), F32),
            pltpu.VMEM((2, 4, 4, 4, 256, 128), BF16),
            pltpu.VMEM((2, 4, 3, 4, 256, 128), BF16),
            pltpu.VMEM((ROWS, 128), F32),
            pltpu.VMEM((2, 2, ROWS, 128), F32),
            pltpu.VMEM((2, 2, ROWS // 2, 128), F32),
            pltpu.VMEM((2, STEPS - PRE, 3, ROWS, 128), BF16),
            pltpu.VMEM((2, STEPS - PRE, 2, ROWS // 2, 128), BF16),
            pltpu.VMEM((2, STEPS - PRE, 2, ROWS, 128), BF16),
            pltpu.VMEM((2, STEPS - PRE, ROWS, 128), BF16),
            pltpu.VMEM((2, STEPS - PRE, ROWS, 128), BF16),
            pltpu.VMEM((2, PRE, 4, ROWS, 128), BF16),
            pltpu.VMEM((2, PRE, 4, ROWS, 128), BF16),
            pltpu.VMEM((2, 4, 4, 4, 2, 128), jnp.int32),
            pltpu.VMEM((2, 4, 4, 4, 2, 128), jnp.int32),
            pltpu.VMEM((32, 128), F32),
            pltpu.VMEM((16, 128), F32),
            dma((4, 4)), dma((2, 4, 3)), dma((2, 4, 3)), dma((2, 4, 2)), dma((2, 4, 2)),
            dma((2, 4, 2, 2)), dma((2, 4, 2, 2)), dma((2, 4, 2)), dma((2, 4, 2)),
            dma((2, PRE, 4)), dma((2, PRE, 4)),
            dma((7,)), dma((7,)), dma((2, 3)), dma((2, 3)), dma, dma, dma,
            pltpu.SemaphoreType.REGULAR, pltpu.SemaphoreType.REGULAR,
        ],
        compiler_params=pltpu.CompilerParams(
            collective_id=0, has_side_effects=True, vmem_limit_bytes=64_000_000),
    )(grad_out, idx, hot_ids)
    return pl.pallas_call(
        outputs,
        out_shape=(jax.ShapeDtypeStruct((1, 1, ROWS, 128), F32), jax.ShapeDtypeStruct((1, 16, 128), F32)),
        in_specs=[vmem, vmem, vmem, smem, smem],
        out_specs=(vmem, vmem),
    )(sums, hot_sums, projections, widths, hot_ids)


def solution(mesh):
    placed = (
        P(("rep", "tab"), None, None),
        P("tab", "rep"),
        P("tab", None, None),
        P(),
        P("tab", None),
    )
    return jax.shard_map(
        shards,
        mesh=mesh,
        in_specs=placed,
        out_specs=(P("rep", "tab", None, None), P("tab", "rep", None)),
        check_vma=False,
    )
```

```python
import jax
import jax.numpy as jnp
from jax import lax
from jax.experimental import pallas as pl
from jax.experimental.pallas import tpu as pltpu
from jax.sharding import PartitionSpec as P

ROWS = 1024
NX, NY, NZ = 4, 4, 8
STEPS = 4
PIECE = 256
PRE = 1
F32 = jnp.float32
BF16 = jnp.bfloat16


def kernel(grad_ref, idx_ref, hot_ref, sums_ref, hotsum_ref,
           stage, tmp, turn, raw, fsum, own, joined, far, part, leaf, near, zsend, zrecv, early, before,
           zi, pi, hot_all, hot_got,
           load_sem, raw_s, raw_r, leaf_s, leaf_r, near_s, near_r, z_s, z_r, early_s, early_r,
           iz_s, iz_r, iq_s, iq_r, hot_s, hot_r, own_sem, round_a, round_b):
    rep = lax.axis_index("rep")
    tab = lax.axis_index("tab")
    x = tab % NX
    z = (tab // NX) % NZ
    y = tab // (NX * NZ)

    def at(px, py, pz):
        return {"tab": (py * NZ + pz) * NX + px}

    def peer(mode, along, shift):
        on_y = (1 - along) * (1 - mode) + along * mode
        return at((x + (1 - on_y) * shift) % NX, (y + on_y * shift) % NY, z)

    def remote(src, dst, s, r, dev):
        return pltpu.make_async_remote_copy(
            src_ref=src, dst_ref=dst, send_sem=s, recv_sem=r,
            device_id=dev, device_id_type=pl.DeviceIdType.MESH)

    def home_of(mode):
        return (z + mode + 1) % 2

    def offset_of(mode, step):
        home = 4 - 2 * step + (step // 2) * (6 + 4 * (step % 2))
        return home_of(mode) * home + (1 - home_of(mode)) * (7 - home)

    def pair_of(mode, step):
        return ((z + offset_of(mode, step) + 8) % NZ) // 2

    def nth_pair(n):
        return (z // 2 + 2 + 3 * n + 3 * (n // 2) + 2 * (n // 3) + 4) % 4

    def load(n, d):
        tile = ((y + d) % NY) * 4 + nth_pair(n)
        return pltpu.make_async_copy(
            grad_ref.at[:, pl.ds(pl.multiple_of(tile * 8, 8), 8), :],
            stage.at[n, d], load_sem.at[n, d])

    def start_loads(i, c):
        load(i // 4, i % 4).start()
        return c

    lax.fori_loop(0, 8, start_loads, 0)

    barrier = pltpu.get_barrier_semaphore()

    def greet(dev):
        pl.semaphore_signal(barrier, inc=1, device_id=dev, device_id_type=pl.DeviceIdType.MESH)

    for d in range(1, 4):
        greet(at((x + d) % NX, y, z))
        greet(at(x, (y + d) % NY, z))
    for d in (1, 7):
        greet(at(x, y, (z + d) % NZ))
    greet({"rep": 1 - rep})
    pl.semaphore_wait(barrier, 9)
    lax.fori_loop(8, 16, start_loads, 0)

    def raw_copy(mode, step, d):
        pos = y * (1 - mode) + x * mode
        return remote(turn.at[mode, pair_of(mode, step), (pos + d) % 4], raw.at[mode, step, d - 1],
                      raw_s.at[mode, step, d - 1], raw_r.at[mode, step, d - 1], peer(mode, 0, d))

    def relayout(i, c):
        n = i // 4
        d = i % 4
        load(n, d).wait()
        tmp[...] = stage[n, d].astype(F32).reshape(2048, 128)
        to_y = (y + d) % NY
        pair = nth_pair(n)
        for px in range(4):
            turn[0, pair, to_y, px] = tmp[pl.ds(px, 256, stride=8), :].astype(BF16)
        for px in range(4):
            turn[1, pair, px, to_y] = tmp[pl.ds(4 + px, 256, stride=8), :].astype(BF16)
        return c

    def send_raw(step):
        def send(i, c):
            raw_copy(i % 2, step, i // 2 + 1).start()
            return c

        lax.fori_loop(0, 6, send, 0)

    lax.fori_loop(0, 8, relayout, 0)
    send_raw(0)

    for sem, away in ((round_a, 1), (round_b, 2)):
        for d in (away, 8 - away):
            pl.semaphore_signal(sem, inc=1, device_id=at(x, y, (z + d) % NZ), device_id_type=pl.DeviceIdType.MESH)
        pl.semaphore_wait(sem, 2)

    def iz(d):
        to = (z + d) % NZ
        return remote(idx_ref.at[:, to], zi.at[z % 2, z // 2], iz_s.at[d - 1], iz_r.at[d - 1], at(x, y, to))

    for d in range(1, 8):
        iz(d).start()
    own_idx = pltpu.make_async_copy(idx_ref.at[:, z], zi.at[z % 2, z // 2], own_sem)
    own_idx.start()
    lax.fori_loop(8, 16, relayout, 0)
    own_idx.wait()

    def iq(mode, d):
        pos = x * (1 - mode) + y * mode
        to = (pos + d) % 4
        return remote(zi.at[0, :, :, to] if mode == 0 else zi.at[1, :, to], pi.at[mode, :, pos],
                      iq_s.at[mode, d - 1], iq_r.at[mode, d - 1], peer(mode, 1, d))

    for d in range(1, 8):
        iz(d).wait()
    for mode in range(2):
        for d in range(1, 4):
            iq(mode, d).start()
    send_raw(1)
    pi[0, :, x] = zi[0, :, :, x]
    pi[1, :, y] = zi[1, :, y]
    for mode in range(2):
        for d in range(1, 4):
            iq(mode, d).wait()

    rows = lax.broadcasted_iota(jnp.int32, (ROWS, 128), 0)

    def onehot(ids, src):
        halves = []
        for h in range(2):
            line = pi[ids + (src, pl.ds(h, 1), slice(None))]
            halves.append(jnp.where(rows == line, F32(1), F32(0)).astype(BF16))
        return jnp.concatenate(halves, axis=1)

    def table_sum(mode, step, dest):
        pos = y * (1 - mode) + x * mode
        pair = pair_of(mode, step)
        values = jnp.concatenate([turn[mode, pair, pos, dest]] + [raw[mode, step, d - 1, dest] for d in range(1, 4)], axis=0)
        ones = jnp.concatenate([onehot((mode, pair, dest), (pos + 4 - d) % 4) for d in range(4)], axis=1)
        fsum[...] = jnp.dot(ones, values, preferred_element_type=F32)

    HALF = ROWS // 2

    def half(h):
        return pl.ds(pl.multiple_of(h * HALF, HALF), HALF)

    def piece(p):
        return pl.ds(pl.multiple_of(p * PIECE, PIECE), PIECE)

    def leaf_copy(mode, side, p):
        return remote(far.at[mode, piece(2 * side + p)], leaf.at[mode, piece(2 * side + p)],
                      leaf_s.at[mode, side, p], leaf_r.at[mode, side, p], peer(mode, 1, 1 + 2 * side))

    def near_copy(mode, step, side, p):
        return remote(part.at[mode, step - PRE, side, piece(p)], near.at[mode, step - PRE, side, piece(p)],
                      near_s.at[mode, step - PRE, side, p], near_r.at[mode, step - PRE, side, p], peer(mode, 1, 1 + 2 * side))

    def along_z(mode, step):
        return at(x, y, (z + 1 + 6 * ((home_of(mode) + step) % 2)) % NZ)

    def z_copy(mode, step, p):
        return remote(zsend.at[mode, step - PRE, piece(p)], zrecv.at[mode, step - PRE, piece(p)],
                      z_s.at[mode, step - PRE, p], z_r.at[mode, step - PRE, p], along_z(mode, step))

    def early_copy(mode, step, dest):
        return remote(early.at[mode, step, dest], before.at[mode, step, dest],
                      early_s.at[mode, step, dest], early_r.at[mode, step, dest], along_z(mode, step))

    def step_body(step, c):
        def arrive(i, c):
            raw_copy(i % 2, step, i // 2 + 1).wait_recv()
            return c

        lax.fori_loop(0, 6, arrive, 0)

        def table(i, c):
            mode = i % 2
            j = (i // 2 + (step // 2) * (1 - step % 2)) % 4
            pos = x * (1 - mode) + y * mode
            shift = (2 + 3 * j + (j // 2) * (3 - 2 * (j % 2))) % 4
            dest = (pos + shift) % 4
            table_sum(mode, step, dest)

            @pl.when((step >= 1) & ((step <= PRE) | (j == 0)))
            def _():
                early_copy(mode, step - 1, dest).wait_recv()
                fsum[...] += before[mode, step - 1, dest].astype(F32)

            @pl.when((step < PRE) | ((j == 0) & (step < STEPS - 1)))
            def _():
                early[mode, step, dest] = fsum[...].astype(BF16)
                early_copy(mode, step, dest).start()

            @pl.when((j == 0) & (step == STEPS - 1))
            def _():
                far[mode] = fsum[...].astype(BF16)
                for p in range(2):
                    leaf_copy(mode, 0, p).start()
                    leaf_copy(mode, 1, p).start()

            @pl.when((i == 1) & (step < STEPS - 2))
            def _():
                send_raw(step + 2)

            @pl.when(((j == 1) | (j == 2)) & (step >= PRE) & (step < STEPS - 1))
            def _():
                part[mode, step - PRE, j - 1] = fsum[...].astype(BF16)
                for p in range(4):
                    near_copy(mode, step, j - 1, p).start()

            @pl.when(((j == 1) | (j == 2)) & (step == STEPS - 1))
            def _():
                side = j - 1
                free = half(1 - side)
                part[mode, step - PRE, side, free] = fsum[free, :].astype(BF16)
                for p in range(2):
                    near_copy(mode, step, side, 2 * (1 - side) + p).start()
                joined[mode, side] = fsum[half(side), :]

            @pl.when((j == 3) & (step >= PRE))
            def _():
                own[mode, step % 2] = fsum[...]

            return c

        lax.fori_loop(0, 8, table, 0)

        @pl.when(step > PRE)
        def _():
            finish(step - 1)

        return c

    def join(i, c):
        mode = i % 2
        side = (i // 2) % 2
        p = i // 4
        at_piece = piece(2 * side + p)
        leaf_copy(mode, side, p).wait_recv()
        part[mode, STEPS - 1 - PRE, side, at_piece] = (
            joined[mode, side, piece(p)] + leaf[mode, at_piece].astype(F32)).astype(BF16)
        near_copy(mode, STEPS - 1, side, 2 * side + p).start()
        return c

    def finish(step):
        def one(i, c):
            mode = (1 + z + i) % 2
            p = (i // 2) // 2 + 2 * ((i // 2) % 2)
            rows_p = piece(p)
            near_copy(mode, step, 0, p).wait_recv()
            near_copy(mode, step, 1, p).wait_recv()
            fsum[rows_p, :] = (own[mode, step % 2, rows_p, :] + near[mode, step - PRE, 0, rows_p, :].astype(F32)
                               + near[mode, step - PRE, 1, rows_p, :].astype(F32))

            @pl.when(step > PRE)
            def _():
                z_copy(mode, step - 1, p).wait_recv()
                fsum[rows_p, :] += zrecv[mode, step - 1 - PRE, rows_p, :].astype(F32)

            @pl.when((home_of(mode) == 0) | (step < STEPS - 1))
            def _():
                zsend[mode, step - PRE, rows_p, :] = fsum[rows_p, :].astype(BF16)
                z_copy(mode, step, p).start()

            return c

        lax.fori_loop(0, 8, one, 0)

    lax.fori_loop(0, STEPS, step_body, 0)
    lax.fori_loop(0, 8, join, 0)
    finish(STEPS - 1)

    for p in (0, 2, 1, 3):
        z_copy(z % 2, STEPS - 1, p).wait_recv()
        sums_ref[piece(p), :] = fsum[piece(p), :] + zrecv[z % 2, STEPS - 1 - PRE, piece(p), :].astype(F32)

    for h in range(32):
        hot_all[pl.ds(h, 1), :] = sums_ref[pl.ds(hot_ref[0, h], 1), :]
    give = remote(hot_all.at[pl.ds(pl.multiple_of((1 - rep) * 16, 16), 16)], hot_got, hot_s, hot_r, {"rep": 1 - rep})
    give.start()

    def drain(i, c):
        mode = i % 2
        step = i // 2
        for d in range(1, 4):
            raw_copy(mode, step, d).wait_send()

        @pl.when(step < PRE)
        def _():
            for dest in range(4):
                early_copy(mode, step, dest).wait_send()

        @pl.when((step >= PRE) & (step < STEPS - 1))
        def _():
            pos = x * (1 - mode) + y * mode
            early_copy(mode, step, (pos + 2) % 4).wait_send()

        @pl.when(step >= PRE)
        def _():
            for side in range(2):
                for p in range(4):
                    near_copy(mode, step, side, p).wait_send()

        @pl.when(step == STEPS - 1)
        def _():
            for side in range(2):
                for p in range(2):
                    leaf_copy(mode, side, p).wait_send()

        @pl.when((step >= PRE) & ((home_of(mode) == 0) | (step < STEPS - 1)))
        def _():
            for p in range(4):
                z_copy(mode, step, p).wait_send()

        return c

    lax.fori_loop(0, 8, drain, 0)
    give.wait()
    hotsum_ref[...] = hot_all[pl.ds(pl.multiple_of(rep * 16, 16), 16), :] + hot_got[...]


def outputs(sums_ref, hotsum_ref, proj_ref, widths_ref, hot_ref, cold_ref, hotout_ref):
    width = widths_ref[lax.axis_index("tab")]
    weights = proj_ref[0]

    def project(total):
        high = total.astype(BF16)
        low = (total - high.astype(F32)).astype(BF16)
        full = (jnp.dot(high, weights, preferred_element_type=F32)
                + jnp.dot(low, weights, preferred_element_type=F32))
        return jnp.where(lax.broadcasted_iota(jnp.int32, full.shape, 1) < width, full, 0.0)

    cold_ref[0, 0] = project(sums_ref[...])
    for h in range(32):
        cold_ref[0, 0, pl.ds(hot_ref[0, h], 1), :] = jnp.zeros((1, 128), F32)
    hotout_ref[0] = project(hotsum_ref[...])


def shards(grad_out, indices, projections, widths, hot_ids):
    idx = indices.reshape(NY, NZ, NX, 2, 128)
    vmem = pl.BlockSpec(memory_space=pltpu.VMEM)
    smem = pl.BlockSpec(memory_space=pltpu.SMEM)
    dma = pltpu.SemaphoreType.DMA
    sums, hot_sums = pl.pallas_call(
        kernel,
        out_shape=(jax.ShapeDtypeStruct((ROWS, 128), F32), jax.ShapeDtypeStruct((16, 128), F32)),
        in_specs=[pl.BlockSpec(memory_space=pl.ANY), pl.BlockSpec(memory_space=pl.ANY), smem],
        out_specs=(vmem, vmem),
        scratch_shapes=[
            pltpu.VMEM((4, 4, 256, 8, 128), BF16),
            pltpu.VMEM((2048, 128), F32),
            pltpu.VMEM((2, 4, 4, 4, 256, 128), BF16),
            pltpu.VMEM((2, 4, 3, 4, 256, 128), BF16),
            pltpu.VMEM((ROWS, 128), F32),
            pltpu.VMEM((2, 2, ROWS, 128), F32),
            pltpu.VMEM((2, 2, ROWS // 2, 128), F32),
            pltpu.VMEM((2, ROWS, 128), BF16),
            pltpu.VMEM((2, STEPS - PRE, 2, ROWS, 128), BF16),
            pltpu.VMEM((2, ROWS, 128), BF16),
            pltpu.VMEM((2, STEPS - PRE, 2, ROWS, 128), BF16),
            pltpu.VMEM((2, STEPS - PRE, ROWS, 128), BF16),
            pltpu.VMEM((2, STEPS - PRE, ROWS, 128), BF16),
            pltpu.VMEM((2, STEPS - 1, 4, ROWS, 128), BF16),
            pltpu.VMEM((2, STEPS - 1, 4, ROWS, 128), BF16),
            pltpu.VMEM((2, 4, 4, 4, 2, 128), jnp.int32),
            pltpu.VMEM((2, 4, 4, 4, 2, 128), jnp.int32),
            pltpu.VMEM((32, 128), F32),
            pltpu.VMEM((16, 128), F32),
            dma((4, 4)), dma((2, 4, 3)), dma((2, 4, 3)), dma((2, 2, 2)), dma((2, 2, 2)),
            dma((2, STEPS - PRE, 2, 4)), dma((2, STEPS - PRE, 2, 4)), dma((2, STEPS - PRE, 4)), dma((2, STEPS - PRE, 4)),
            dma((2, STEPS - 1, 4)), dma((2, STEPS - 1, 4)),
            dma((7,)), dma((7,)), dma((2, 3)), dma((2, 3)), dma, dma, dma,
            pltpu.SemaphoreType.REGULAR, pltpu.SemaphoreType.REGULAR,
        ],
        compiler_params=pltpu.CompilerParams(
            collective_id=0, has_side_effects=True, vmem_limit_bytes=64_000_000),
    )(grad_out, idx, hot_ids)
    return pl.pallas_call(
        outputs,
        out_shape=(jax.ShapeDtypeStruct((1, 1, ROWS, 128), F32), jax.ShapeDtypeStruct((1, 16, 128), F32)),
        in_specs=[vmem, vmem, vmem, smem, smem],
        out_specs=(vmem, vmem),
    )(sums, hot_sums, projections, widths, hot_ids)


def solution(mesh):
    placed = (
        P(("rep", "tab"), None, None),
        P("tab", "rep"),
        P("tab", None, None),
        P(),
        P("tab", None),
    )
    return jax.shard_map(
        shards,
        mesh=mesh,
        in_specs=placed,
        out_specs=(P("rep", "tab", None, None), P("tab", "rep", None)),
        check_vma=False,
    )
```

```python
import jax
import jax.numpy as jnp
from jax import lax
from jax.experimental import pallas as pl
from jax.experimental.pallas import tpu as pltpu
from jax.sharding import PartitionSpec as P

ROWS = 1024
NX, NY, NZ = 4, 4, 8
STEPS = 4
PIECE = 256
PRE = 1
F32 = jnp.float32
BF16 = jnp.bfloat16


def kernel(grad_ref, idx_ref, hot_ref, sums_ref, hotsum_ref,
           stage, tmp, turn, raw, fsum, own, joined, far, part, leaf, near, zsend, zrecv, early, before,
           zi, pi, hot_all, hot_got,
           load_sem, raw_s, raw_r, leaf_s, leaf_r, near_s, near_r, z_s, z_r, early_s, early_r,
           iz_s, iz_r, iq_s, iq_r, hot_s, hot_r, own_sem, round_a, round_b):
    rep = lax.axis_index("rep")
    tab = lax.axis_index("tab")
    x = tab % NX
    z = (tab // NX) % NZ
    y = tab // (NX * NZ)

    def at(px, py, pz):
        return {"tab": (py * NZ + pz) * NX + px}

    def peer(mode, along, shift):
        on_y = (1 - along) * (1 - mode) + along * mode
        return at((x + (1 - on_y) * shift) % NX, (y + on_y * shift) % NY, z)

    def remote(src, dst, s, r, dev):
        return pltpu.make_async_remote_copy(
            src_ref=src, dst_ref=dst, send_sem=s, recv_sem=r,
            device_id=dev, device_id_type=pl.DeviceIdType.MESH)

    def home_of(mode):
        return (z + mode + 1) % 2

    def offset_of(mode, step):
        home = 4 - 2 * step + (step // 2) * (6 + 4 * (step % 2))
        return home_of(mode) * home + (1 - home_of(mode)) * (7 - home)

    def pair_of(mode, step):
        return ((z + offset_of(mode, step) + 8) % NZ) // 2

    def nth_pair(n):
        return (z // 2 + 2 + 3 * n + 3 * (n // 2) + 2 * (n // 3) + 4) % 4

    def load(n, d):
        tile = ((y + d) % NY) * 4 + nth_pair(n)
        return pltpu.make_async_copy(
            grad_ref.at[:, pl.ds(pl.multiple_of(tile * 8, 8), 8), :],
            stage.at[n, d], load_sem.at[n, d])

    def start_loads(i, c):
        load(i // 4, i % 4).start()
        return c

    lax.fori_loop(0, 8, start_loads, 0)

    barrier = pltpu.get_barrier_semaphore()

    def greet(dev):
        pl.semaphore_signal(barrier, inc=1, device_id=dev, device_id_type=pl.DeviceIdType.MESH)

    for d in range(1, 4):
        greet(at((x + d) % NX, y, z))
        greet(at(x, (y + d) % NY, z))
    for d in (1, 7):
        greet(at(x, y, (z + d) % NZ))
    greet({"rep": 1 - rep})
    pl.semaphore_wait(barrier, 9)
    lax.fori_loop(8, 16, start_loads, 0)

    def raw_copy(mode, step, d):
        pos = y * (1 - mode) + x * mode
        return remote(turn.at[mode, pair_of(mode, step), (pos + d) % 4], raw.at[mode, step, d - 1],
                      raw_s.at[mode, step, d - 1], raw_r.at[mode, step, d - 1], peer(mode, 0, d))

    def relayout(i, c):
        n = i // 4
        d = i % 4
        load(n, d).wait()
        tmp[...] = stage[n, d].astype(F32).reshape(2048, 128)
        to_y = (y + d) % NY
        pair = nth_pair(n)
        for px in range(4):
            turn[0, pair, to_y, px] = tmp[pl.ds(px, 256, stride=8), :].astype(BF16)
        for px in range(4):
            turn[1, pair, px, to_y] = tmp[pl.ds(4 + px, 256, stride=8), :].astype(BF16)
        return c

    def send_raw(step):
        def send(i, c):
            raw_copy(i % 2, step, i // 2 + 1).start()
            return c

        lax.fori_loop(0, 6, send, 0)

    lax.fori_loop(0, 8, relayout, 0)
    send_raw(0)

    for sem, away in ((round_a, 1), (round_b, 2)):
        for d in (away, 8 - away):
            pl.semaphore_signal(sem, inc=1, device_id=at(x, y, (z + d) % NZ), device_id_type=pl.DeviceIdType.MESH)
        pl.semaphore_wait(sem, 2)

    def iz(d):
        to = (z + d) % NZ
        return remote(idx_ref.at[:, to], zi.at[z % 2, z // 2], iz_s.at[d - 1], iz_r.at[d - 1], at(x, y, to))

    for d in range(1, 8):
        iz(d).start()
    own_idx = pltpu.make_async_copy(idx_ref.at[:, z], zi.at[z % 2, z // 2], own_sem)
    own_idx.start()
    lax.fori_loop(8, 16, relayout, 0)
    own_idx.wait()

    def iq(mode, d):
        pos = x * (1 - mode) + y * mode
        to = (pos + d) % 4
        return remote(zi.at[0, :, :, to] if mode == 0 else zi.at[1, :, to], pi.at[mode, :, pos],
                      iq_s.at[mode, d - 1], iq_r.at[mode, d - 1], peer(mode, 1, d))

    for d in range(1, 8):
        iz(d).wait()
    for mode in range(2):
        for d in range(1, 4):
            iq(mode, d).start()
    send_raw(1)
    pi[0, :, x] = zi[0, :, :, x]
    pi[1, :, y] = zi[1, :, y]
    for mode in range(2):
        for d in range(1, 4):
            iq(mode, d).wait()

    rows = lax.broadcasted_iota(jnp.int32, (ROWS, 128), 0)

    def onehot(ids, src):
        halves = []
        for h in range(2):
            line = pi[ids + (src, pl.ds(h, 1), slice(None))]
            halves.append(jnp.where(rows == line, F32(1), F32(0)).astype(BF16))
        return jnp.concatenate(halves, axis=1)

    def table_sum(mode, step, dest):
        pos = y * (1 - mode) + x * mode
        pair = pair_of(mode, step)
        values = jnp.concatenate([turn[mode, pair, pos, dest]] + [raw[mode, step, d - 1, dest] for d in range(1, 4)], axis=0)
        ones = jnp.concatenate([onehot((mode, pair, dest), (pos + 4 - d) % 4) for d in range(4)], axis=1)
        fsum[...] = jnp.dot(ones, values, preferred_element_type=F32)

    HALF = ROWS // 2

    def half(h):
        return pl.ds(pl.multiple_of(h * HALF, HALF), HALF)

    def piece(p):
        return pl.ds(pl.multiple_of(p * PIECE, PIECE), PIECE)

    def leaf_copy(mode, side, p):
        return remote(far.at[mode, piece(2 * side + p)], leaf.at[mode, piece(2 * side + p)],
                      leaf_s.at[mode, side, p], leaf_r.at[mode, side, p], peer(mode, 1, 1 + 2 * side))

    def near_copy(mode, step, side, p):
        return remote(part.at[mode, step - PRE, side, piece(p)], near.at[mode, step - PRE, side, piece(p)],
                      near_s.at[mode, step - PRE, side, p], near_r.at[mode, step - PRE, side, p], peer(mode, 1, 1 + 2 * side))

    def along_z(mode, step):
        return at(x, y, (z + 1 + 6 * ((home_of(mode) + step) % 2)) % NZ)

    def z_copy(mode, step, p):
        return remote(zsend.at[mode, step - PRE, piece(p)], zrecv.at[mode, step - PRE, piece(p)],
                      z_s.at[mode, step - PRE, p], z_r.at[mode, step - PRE, p], along_z(mode, step))

    def early_copy(mode, step, dest):
        return remote(early.at[mode, step, dest], before.at[mode, step, dest],
                      early_s.at[mode, step, dest], early_r.at[mode, step, dest], along_z(mode, step))

    def step_body(step, c):
        def arrive(i, c):
            raw_copy(i % 2, step, i // 2 + 1).wait_recv()
            return c

        lax.fori_loop(0, 6, arrive, 0)

        def table(i, c):
            mode = i % 2
            j = (i // 2 + (step // 2) * (1 - step % 2)) % 4
            pos = x * (1 - mode) + y * mode
            shift = (2 + 3 * j + (j // 2) * (3 - 2 * (j % 2))) % 4
            dest = (pos + shift) % 4
            table_sum(mode, step, dest)

            @pl.when((step >= 1) & ((step <= PRE) | (j == 0)))
            def _():
                early_copy(mode, step - 1, dest).wait_recv()
                fsum[...] += before[mode, step - 1, dest].astype(F32)

            @pl.when((step < PRE) | ((j == 0) & (step < STEPS - 1)))
            def _():
                early[mode, step, dest] = fsum[...].astype(BF16)
                early_copy(mode, step, dest).start()

            @pl.when((j == 0) & (step == STEPS - 1))
            def _():
                far[mode] = fsum[...].astype(BF16)
                for p in range(2):
                    leaf_copy(mode, 0, p).start()
                    leaf_copy(mode, 1, p).start()

            @pl.when((i == 1 + 4 * step) & (step < STEPS - 2))
            def _():
                send_raw(step + 2)

            @pl.when(((j == 1) | (j == 2)) & (step >= PRE) & (step < STEPS - 1))
            def _():
                part[mode, step - PRE, j - 1] = fsum[...].astype(BF16)
                for p in range(4):
                    near_copy(mode, step, j - 1, p).start()

            @pl.when(((j == 1) | (j == 2)) & (step == STEPS - 1))
            def _():
                side = j - 1
                free = half(1 - side)
                part[mode, step - PRE, side, free] = fsum[free, :].astype(BF16)
                for p in range(2):
                    near_copy(mode, step, side, 2 * (1 - side) + p).start()
                joined[mode, side] = fsum[half(side), :]

            @pl.when((j == 3) & (step >= PRE))
            def _():
                own[mode, step % 2] = fsum[...]

            return c

        lax.fori_loop(0, 8, table, 0)

        @pl.when(step > PRE)
        def _():
            finish(step - 1)

        return c

    def join(i, c):
        mode = i % 2
        side = (i // 2) % 2
        p = i // 4
        at_piece = piece(2 * side + p)
        leaf_copy(mode, side, p).wait_recv()
        part[mode, STEPS - 1 - PRE, side, at_piece] = (
            joined[mode, side, piece(p)] + leaf[mode, at_piece].astype(F32)).astype(BF16)
        near_copy(mode, STEPS - 1, side, 2 * side + p).start()
        return c

    def finish(step):
        def one(i, c):
            mode = (1 + z + i) % 2
            p = (i // 2) // 2 + 2 * ((i // 2) % 2)
            rows_p = piece(p)
            near_copy(mode, step, 0, p).wait_recv()
            near_copy(mode, step, 1, p).wait_recv()
            fsum[rows_p, :] = (own[mode, step % 2, rows_p, :] + near[mode, step - PRE, 0, rows_p, :].astype(F32)
                               + near[mode, step - PRE, 1, rows_p, :].astype(F32))

            @pl.when(step > PRE)
            def _():
                z_copy(mode, step - 1, p).wait_recv()
                fsum[rows_p, :] += zrecv[mode, step - 1 - PRE, rows_p, :].astype(F32)

            @pl.when((home_of(mode) == 0) | (step < STEPS - 1))
            def _():
                zsend[mode, step - PRE, rows_p, :] = fsum[rows_p, :].astype(BF16)
                z_copy(mode, step, p).start()

            return c

        lax.fori_loop(0, 8, one, 0)

    lax.fori_loop(0, STEPS, step_body, 0)
    lax.fori_loop(0, 8, join, 0)
    finish(STEPS - 1)

    for p in (0, 2, 1, 3):
        z_copy(z % 2, STEPS - 1, p).wait_recv()
        sums_ref[piece(p), :] = fsum[piece(p), :] + zrecv[z % 2, STEPS - 1 - PRE, piece(p), :].astype(F32)

    for h in range(32):
        hot_all[pl.ds(h, 1), :] = sums_ref[pl.ds(hot_ref[0, h], 1), :]
    give = remote(hot_all.at[pl.ds(pl.multiple_of((1 - rep) * 16, 16), 16)], hot_got, hot_s, hot_r, {"rep": 1 - rep})
    give.start()

    def drain(i, c):
        mode = i % 2
        step = i // 2
        for d in range(1, 4):
            raw_copy(mode, step, d).wait_send()

        @pl.when(step < PRE)
        def _():
            for dest in range(4):
                early_copy(mode, step, dest).wait_send()

        @pl.when((step >= PRE) & (step < STEPS - 1))
        def _():
            pos = x * (1 - mode) + y * mode
            early_copy(mode, step, (pos + 2) % 4).wait_send()

        @pl.when(step >= PRE)
        def _():
            for side in range(2):
                for p in range(4):
                    near_copy(mode, step, side, p).wait_send()

        @pl.when(step == STEPS - 1)
        def _():
            for side in range(2):
                for p in range(2):
                    leaf_copy(mode, side, p).wait_send()

        @pl.when((step >= PRE) & ((home_of(mode) == 0) | (step < STEPS - 1)))
        def _():
            for p in range(4):
                z_copy(mode, step, p).wait_send()

        return c

    lax.fori_loop(0, 8, drain, 0)
    give.wait()
    hotsum_ref[...] = hot_all[pl.ds(pl.multiple_of(rep * 16, 16), 16), :] + hot_got[...]


def outputs(sums_ref, hotsum_ref, proj_ref, widths_ref, hot_ref, cold_ref, hotout_ref):
    width = widths_ref[lax.axis_index("tab")]
    weights = proj_ref[0]

    def project(total):
        high = total.astype(BF16)
        low = (total - high.astype(F32)).astype(BF16)
        full = (jnp.dot(high, weights, preferred_element_type=F32)
                + jnp.dot(low, weights, preferred_element_type=F32))
        return jnp.where(lax.broadcasted_iota(jnp.int32, full.shape, 1) < width, full, 0.0)

    cold_ref[0, 0] = project(sums_ref[...])
    for h in range(32):
        cold_ref[0, 0, pl.ds(hot_ref[0, h], 1), :] = jnp.zeros((1, 128), F32)
    hotout_ref[0] = project(hotsum_ref[...])


def shards(grad_out, indices, projections, widths, hot_ids):
    idx = indices.reshape(NY, NZ, NX, 2, 128)
    vmem = pl.BlockSpec(memory_space=pltpu.VMEM)
    smem = pl.BlockSpec(memory_space=pltpu.SMEM)
    dma = pltpu.SemaphoreType.DMA
    sums, hot_sums = pl.pallas_call(
        kernel,
        out_shape=(jax.ShapeDtypeStruct((ROWS, 128), F32), jax.ShapeDtypeStruct((16, 128), F32)),
        in_specs=[pl.BlockSpec(memory_space=pl.ANY), pl.BlockSpec(memory_space=pl.ANY), smem],
        out_specs=(vmem, vmem),
        scratch_shapes=[
            pltpu.VMEM((4, 4, 256, 8, 128), BF16),
            pltpu.VMEM((2048, 128), F32),
            pltpu.VMEM((2, 4, 4, 4, 256, 128), BF16),
            pltpu.VMEM((2, 4, 3, 4, 256, 128), BF16),
            pltpu.VMEM((ROWS, 128), F32),
            pltpu.VMEM((2, 2, ROWS, 128), F32),
            pltpu.VMEM((2, 2, ROWS // 2, 128), F32),
            pltpu.VMEM((2, ROWS, 128), BF16),
            pltpu.VMEM((2, STEPS - PRE, 2, ROWS, 128), BF16),
            pltpu.VMEM((2, ROWS, 128), BF16),
            pltpu.VMEM((2, STEPS - PRE, 2, ROWS, 128), BF16),
            pltpu.VMEM((2, STEPS - PRE, ROWS, 128), BF16),
            pltpu.VMEM((2, STEPS - PRE, ROWS, 128), BF16),
            pltpu.VMEM((2, STEPS - 1, 4, ROWS, 128), BF16),
            pltpu.VMEM((2, STEPS - 1, 4, ROWS, 128), BF16),
            pltpu.VMEM((2, 4, 4, 4, 2, 128), jnp.int32),
            pltpu.VMEM((2, 4, 4, 4, 2, 128), jnp.int32),
            pltpu.VMEM((32, 128), F32),
            pltpu.VMEM((16, 128), F32),
            dma((4, 4)), dma((2, 4, 3)), dma((2, 4, 3)), dma((2, 2, 2)), dma((2, 2, 2)),
            dma((2, STEPS - PRE, 2, 4)), dma((2, STEPS - PRE, 2, 4)), dma((2, STEPS - PRE, 4)), dma((2, STEPS - PRE, 4)),
            dma((2, STEPS - 1, 4)), dma((2, STEPS - 1, 4)),
            dma((7,)), dma((7,)), dma((2, 3)), dma((2, 3)), dma, dma, dma,
            pltpu.SemaphoreType.REGULAR, pltpu.SemaphoreType.REGULAR,
        ],
        compiler_params=pltpu.CompilerParams(
            collective_id=0, has_side_effects=True, vmem_limit_bytes=64_000_000),
    )(grad_out, idx, hot_ids)
    return pl.pallas_call(
        outputs,
        out_shape=(jax.ShapeDtypeStruct((1, 1, ROWS, 128), F32), jax.ShapeDtypeStruct((1, 16, 128), F32)),
        in_specs=[vmem, vmem, vmem, smem, smem],
        out_specs=(vmem, vmem),
    )(sums, hot_sums, projections, widths, hot_ids)


def solution(mesh):
    placed = (
        P(("rep", "tab"), None, None),
        P("tab", "rep"),
        P("tab", None, None),
        P(),
        P("tab", None),
    )
    return jax.shard_map(
        shards,
        mesh=mesh,
        in_specs=placed,
        out_specs=(P("rep", "tab", None, None), P("tab", "rep", None)),
        check_vma=False,
    )
```

```python
import jax
import jax.numpy as jnp
from jax import lax
from jax.experimental import pallas as pl
from jax.experimental.pallas import tpu as pltpu
from jax.sharding import PartitionSpec as P

ROWS = 1024
NX, NY, NZ = 4, 4, 8
STEPS = 4
PIECE = 256
PRE = 1
F32 = jnp.float32
BF16 = jnp.bfloat16


def kernel(grad_ref, idx_ref, hot_ref, sums_ref, hotsum_ref,
           stage, tmp, turn, raw, fsum, own, joined, far, part, leaf, near, zsend, zrecv, early, before,
           zi, pi, hot_all, hot_got,
           load_sem, raw_s, raw_r, leaf_s, leaf_r, near_s, near_r, z_s, z_r, early_s, early_r,
           iz_s, iz_r, iq_s, iq_r, hot_s, hot_r, own_sem, round_a, round_b):
    rep = lax.axis_index("rep")
    tab = lax.axis_index("tab")
    x = tab % NX
    z = (tab // NX) % NZ
    y = tab // (NX * NZ)

    def at(px, py, pz):
        return {"tab": (py * NZ + pz) * NX + px}

    def peer(mode, along, shift):
        on_y = (1 - along) * (1 - mode) + along * mode
        return at((x + (1 - on_y) * shift) % NX, (y + on_y * shift) % NY, z)

    def remote(src, dst, s, r, dev):
        return pltpu.make_async_remote_copy(
            src_ref=src, dst_ref=dst, send_sem=s, recv_sem=r,
            device_id=dev, device_id_type=pl.DeviceIdType.MESH)

    def home_of(mode):
        return (z + mode + 1) % 2

    def offset_of(mode, step):
        home = 4 - 2 * step + (step // 2) * (6 + 4 * (step % 2))
        return home_of(mode) * home + (1 - home_of(mode)) * (7 - home)

    def pair_of(mode, step):
        return ((z + offset_of(mode, step) + 8) % NZ) // 2

    def nth_pair(n):
        return (z // 2 + 2 + 3 * n + 3 * (n // 2) + 2 * (n // 3) + 4) % 4

    def load(n, d):
        tile = ((y + d) % NY) * 4 + nth_pair(n)
        return pltpu.make_async_copy(
            grad_ref.at[:, pl.ds(pl.multiple_of(tile * 8, 8), 8), :],
            stage.at[n, d], load_sem.at[n, d])

    def start_loads(i, c):
        load(i // 4, i % 4).start()
        return c

    lax.fori_loop(0, 8, start_loads, 0)

    barrier = pltpu.get_barrier_semaphore()

    def greet(dev):
        pl.semaphore_signal(barrier, inc=1, device_id=dev, device_id_type=pl.DeviceIdType.MESH)

    for d in range(1, 4):
        greet(at((x + d) % NX, y, z))
        greet(at(x, (y + d) % NY, z))
    for d in (1, 7):
        greet(at(x, y, (z + d) % NZ))
    greet({"rep": 1 - rep})
    pl.semaphore_wait(barrier, 9)
    lax.fori_loop(8, 16, start_loads, 0)

    def raw_copy(mode, step, d):
        pos = y * (1 - mode) + x * mode
        return remote(turn.at[mode, pair_of(mode, step), (pos + d) % 4], raw.at[mode, step, d - 1],
                      raw_s.at[mode, step, d - 1], raw_r.at[mode, step, d - 1], peer(mode, 0, d))

    def relayout(i, c):
        n = i // 4
        d = i % 4
        load(n, d).wait()
        tmp[...] = stage[n, d].astype(F32).reshape(2048, 128)
        to_y = (y + d) % NY
        pair = nth_pair(n)
        for px in range(4):
            turn[0, pair, to_y, px] = tmp[pl.ds(px, 256, stride=8), :].astype(BF16)
        for px in range(4):
            turn[1, pair, px, to_y] = tmp[pl.ds(4 + px, 256, stride=8), :].astype(BF16)
        return c

    def send_raw(step):
        def send(i, c):
            raw_copy(i % 2, step, i // 2 + 1).start()
            return c

        lax.fori_loop(0, 6, send, 0)

    lax.fori_loop(0, 8, relayout, 0)
    send_raw(0)

    for sem, away in ((round_a, 1), (round_b, 2)):
        for d in (away, 8 - away):
            pl.semaphore_signal(sem, inc=1, device_id=at(x, y, (z + d) % NZ), device_id_type=pl.DeviceIdType.MESH)
        pl.semaphore_wait(sem, 2)

    def iz(d):
        to = (z + d) % NZ
        return remote(idx_ref.at[:, to], zi.at[z % 2, z // 2], iz_s.at[d - 1], iz_r.at[d - 1], at(x, y, to))

    for d in range(1, 8):
        iz(d).start()
    own_idx = pltpu.make_async_copy(idx_ref.at[:, z], zi.at[z % 2, z // 2], own_sem)
    own_idx.start()
    lax.fori_loop(8, 16, relayout, 0)
    own_idx.wait()

    def iq(mode, d):
        pos = x * (1 - mode) + y * mode
        to = (pos + d) % 4
        return remote(zi.at[0, :, :, to] if mode == 0 else zi.at[1, :, to], pi.at[mode, :, pos],
                      iq_s.at[mode, d - 1], iq_r.at[mode, d - 1], peer(mode, 1, d))

    for d in range(1, 8):
        iz(d).wait()
    for mode in range(2):
        for d in range(1, 4):
            iq(mode, d).start()
    send_raw(1)
    pi[0, :, x] = zi[0, :, :, x]
    pi[1, :, y] = zi[1, :, y]
    for mode in range(2):
        for d in range(1, 4):
            iq(mode, d).wait()

    rows = lax.broadcasted_iota(jnp.int32, (ROWS, 128), 0)

    def onehot(ids, src):
        halves = []
        for h in range(2):
            line = pi[ids + (src, pl.ds(h, 1), slice(None))]
            halves.append(jnp.where(rows == line, F32(1), F32(0)).astype(BF16))
        return jnp.concatenate(halves, axis=1)

    def table_sum(mode, step, dest):
        pos = y * (1 - mode) + x * mode
        pair = pair_of(mode, step)
        values = jnp.concatenate([turn[mode, pair, pos, dest]] + [raw[mode, step, d - 1, dest] for d in range(1, 4)], axis=0)
        ones = jnp.concatenate([onehot((mode, pair, dest), (pos + 4 - d) % 4) for d in range(4)], axis=1)
        fsum[...] = jnp.dot(ones, values, preferred_element_type=F32)

    HALF = ROWS // 2

    def half(h):
        return pl.ds(pl.multiple_of(h * HALF, HALF), HALF)

    def piece(p):
        return pl.ds(pl.multiple_of(p * PIECE, PIECE), PIECE)

    def leaf_copy(mode, side, p):
        return remote(far.at[mode, piece(2 * side + p)], leaf.at[mode, piece(2 * side + p)],
                      leaf_s.at[mode, side, p], leaf_r.at[mode, side, p], peer(mode, 1, 1 + 2 * side))

    def near_copy(mode, step, side, p):
        return remote(part.at[mode, step - PRE, side, piece(p)], near.at[mode, step - PRE, side, piece(p)],
                      near_s.at[mode, step - PRE, side, p], near_r.at[mode, step - PRE, side, p], peer(mode, 1, 1 + 2 * side))

    def along_z(mode, step):
        return at(x, y, (z + 1 + 6 * ((home_of(mode) + step) % 2)) % NZ)

    def z_copy(mode, step, p):
        return remote(zsend.at[mode, step - PRE, piece(p)], zrecv.at[mode, step - PRE, piece(p)],
                      z_s.at[mode, step - PRE, p], z_r.at[mode, step - PRE, p], along_z(mode, step))

    def early_copy(mode, step, dest):
        return remote(early.at[mode, step, dest], before.at[mode, step, dest],
                      early_s.at[mode, step, dest], early_r.at[mode, step, dest], along_z(mode, step))

    def step_body(step, c):
        def arrive(i, c):
            raw_copy(i % 2, step, i // 2 + 1).wait_recv()
            return c

        lax.fori_loop(0, 6, arrive, 0)

        def table(i, c):
            mode = i % 2
            j = (i // 2 + (step // 2) * (1 - step % 2)) % 4
            pos = x * (1 - mode) + y * mode
            shift = (2 + 3 * j + (j // 2) * (3 - 2 * (j % 2))) % 4
            dest = (pos + shift) % 4
            table_sum(mode, step, dest)

            @pl.when((step >= 1) & ((step <= PRE) | (j == 0)))
            def _():
                early_copy(mode, step - 1, dest).wait_recv()
                fsum[...] += before[mode, step - 1, dest].astype(F32)

            @pl.when((step < PRE) | ((j == 0) & (step < STEPS - 1)))
            def _():
                early[mode, step, dest] = fsum[...].astype(BF16)
                early_copy(mode, step, dest).start()

            @pl.when((j == 0) & (step == STEPS - 1))
            def _():
                far[mode] = fsum[...].astype(BF16)
                for p in range(2):
                    leaf_copy(mode, 0, p).start()
                    leaf_copy(mode, 1, p).start()

            @pl.when((i == 1 + 4 * step) & (step < STEPS - 2))
            def _():
                send_raw(step + 2)

            @pl.when(((j == 1) | (j == 2)) & (step >= PRE) & (step < STEPS - 1))
            def _():
                part[mode, step - PRE, j - 1] = fsum[...].astype(BF16)
                for p in range(4):
                    near_copy(mode, step, j - 1, p).start()

            @pl.when(((j == 1) | (j == 2)) & (step == STEPS - 1))
            def _():
                side = j - 1
                free = half(1 - side)
                part[mode, step - PRE, side, free] = fsum[free, :].astype(BF16)
                for p in range(2):
                    near_copy(mode, step, side, 2 * (1 - side) + p).start()
                joined[mode, side] = fsum[half(side), :]

            @pl.when((j == 3) & (step >= PRE))
            def _():
                own[mode, step % 2] = fsum[...]

            return c

        lax.fori_loop(0, 8, table, 0)

        @pl.when(step > PRE)
        def _():
            finish(step - 1)

        return c

    def join(i, c):
        mode = i % 2
        side = (i // 2) % 2
        p = i // 4
        at_piece = piece(2 * side + p)
        leaf_copy(mode, side, p).wait_recv()
        part[mode, STEPS - 1 - PRE, side, at_piece] = (
            joined[mode, side, piece(p)] + leaf[mode, at_piece].astype(F32)).astype(BF16)
        near_copy(mode, STEPS - 1, side, 2 * side + p).start()
        return c

    def finish(step):
        def one(i, c):
            mode = (1 + z + i) % 2
            p = (i // 2) // 2 + 2 * ((i // 2) % 2)
            rows_p = piece(p)
            near_copy(mode, step, 0, p).wait_recv()
            near_copy(mode, step, 1, p).wait_recv()
            fsum[rows_p, :] = (own[mode, step % 2, rows_p, :] + near[mode, step - PRE, 0, rows_p, :].astype(F32)
                               + near[mode, step - PRE, 1, rows_p, :].astype(F32))

            @pl.when(step > PRE)
            def _():
                z_copy(mode, step - 1, p).wait_recv()
                fsum[rows_p, :] += zrecv[mode, step - 1 - PRE, rows_p, :].astype(F32)

            @pl.when((home_of(mode) == 0) | (step < STEPS - 1))
            def _():
                zsend[mode, step - PRE, rows_p, :] = fsum[rows_p, :].astype(BF16)
                z_copy(mode, step, p).start()

            return c

        lax.fori_loop(0, 8, one, 0)

    lax.fori_loop(0, STEPS, step_body, 0)
    lax.fori_loop(0, 8, join, 0)
    finish(STEPS - 1)

    for p in (0, 2, 1, 3):
        z_copy(z % 2, STEPS - 1, p).wait_recv()
        sums_ref[piece(p), :] = fsum[piece(p), :] + zrecv[z % 2, STEPS - 1 - PRE, piece(p), :].astype(F32)

    for h in range(32):
        hot_all[pl.ds(h, 1), :] = sums_ref[pl.ds(hot_ref[0, h], 1), :]
    give = remote(hot_all.at[pl.ds(pl.multiple_of((1 - rep) * 16, 16), 16)], hot_got, hot_s, hot_r, {"rep": 1 - rep})
    give.start()

    def drain(i, c):
        mode = i % 2
        step = i // 2
        for d in range(1, 4):
            raw_copy(mode, step, d).wait_send()

        @pl.when(step < PRE)
        def _():
            for dest in range(4):
                early_copy(mode, step, dest).wait_send()

        @pl.when((step >= PRE) & (step < STEPS - 1))
        def _():
            pos = x * (1 - mode) + y * mode
            early_copy(mode, step, (pos + 2) % 4).wait_send()

        @pl.when(step >= PRE)
        def _():
            for side in range(2):
                for p in range(4):
                    near_copy(mode, step, side, p).wait_send()

        @pl.when(step == STEPS - 1)
        def _():
            for side in range(2):
                for p in range(2):
                    leaf_copy(mode, side, p).wait_send()

        @pl.when((step >= PRE) & ((home_of(mode) == 0) | (step < STEPS - 1)))
        def _():
            for p in range(4):
                z_copy(mode, step, p).wait_send()

        return c

    lax.fori_loop(0, 8, drain, 0)
    give.wait()
    hotsum_ref[...] = hot_all[pl.ds(pl.multiple_of(rep * 16, 16), 16), :] + hot_got[...]


def outputs(sums_ref, hotsum_ref, proj_ref, widths_ref, hot_ref, cold_ref, hotout_ref):
    width = widths_ref[lax.axis_index("tab")]
    weights = proj_ref[0]

    def project(total):
        high = total.astype(BF16)
        low = (total - high.astype(F32)).astype(BF16)
        full = (jnp.dot(high, weights, preferred_element_type=F32)
                + jnp.dot(low, weights, preferred_element_type=F32))
        return jnp.where(lax.broadcasted_iota(jnp.int32, full.shape, 1) < width, full, 0.0)

    cold_ref[0, 0] = project(sums_ref[...])
    for h in range(32):
        cold_ref[0, 0, pl.ds(hot_ref[0, h], 1), :] = jnp.zeros((1, 128), F32)
    hotout_ref[0] = project(hotsum_ref[...])


def shards(grad_out, indices, projections, widths, hot_ids):
    idx = indices.reshape(NY, NZ, NX, 2, 128)
    vmem = pl.BlockSpec(memory_space=pltpu.VMEM)
    smem = pl.BlockSpec(memory_space=pltpu.SMEM)
    dma = pltpu.SemaphoreType.DMA
    sums, hot_sums = pl.pallas_call(
        kernel,
        out_shape=(pltpu.VMEM((ROWS, 128), F32), pltpu.VMEM((16, 128), F32)),
        in_specs=[pl.BlockSpec(memory_space=pl.ANY), pl.BlockSpec(memory_space=pl.ANY), smem],
        out_specs=(vmem, vmem),
        scratch_shapes=[
            pltpu.VMEM((4, 4, 256, 8, 128), BF16),
            pltpu.VMEM((2048, 128), F32),
            pltpu.VMEM((2, 4, 4, 4, 256, 128), BF16),
            pltpu.VMEM((2, 4, 3, 4, 256, 128), BF16),
            pltpu.VMEM((ROWS, 128), F32),
            pltpu.VMEM((2, 2, ROWS, 128), F32),
            pltpu.VMEM((2, 2, ROWS // 2, 128), F32),
            pltpu.VMEM((2, ROWS, 128), BF16),
            pltpu.VMEM((2, STEPS - PRE, 2, ROWS, 128), BF16),
            pltpu.VMEM((2, ROWS, 128), BF16),
            pltpu.VMEM((2, STEPS - PRE, 2, ROWS, 128), BF16),
            pltpu.VMEM((2, STEPS - PRE, ROWS, 128), BF16),
            pltpu.VMEM((2, STEPS - PRE, ROWS, 128), BF16),
            pltpu.VMEM((2, STEPS - 1, 4, ROWS, 128), BF16),
            pltpu.VMEM((2, STEPS - 1, 4, ROWS, 128), BF16),
            pltpu.VMEM((2, 4, 4, 4, 2, 128), jnp.int32),
            pltpu.VMEM((2, 4, 4, 4, 2, 128), jnp.int32),
            pltpu.VMEM((32, 128), F32),
            pltpu.VMEM((16, 128), F32),
            dma((4, 4)), dma((2, 4, 3)), dma((2, 4, 3)), dma((2, 2, 2)), dma((2, 2, 2)),
            dma((2, STEPS - PRE, 2, 4)), dma((2, STEPS - PRE, 2, 4)), dma((2, STEPS - PRE, 4)), dma((2, STEPS - PRE, 4)),
            dma((2, STEPS - 1, 4)), dma((2, STEPS - 1, 4)),
            dma((7,)), dma((7,)), dma((2, 3)), dma((2, 3)), dma, dma, dma,
            pltpu.SemaphoreType.REGULAR, pltpu.SemaphoreType.REGULAR,
        ],
        compiler_params=pltpu.CompilerParams(
            collective_id=0, has_side_effects=True, vmem_limit_bytes=60_000_000),
    )(grad_out, idx, hot_ids)
    return pl.pallas_call(
        outputs,
        out_shape=(jax.ShapeDtypeStruct((1, 1, ROWS, 128), F32), jax.ShapeDtypeStruct((1, 16, 128), F32)),
        in_specs=[vmem, vmem, vmem, smem, smem],
        out_specs=(vmem, vmem),
        compiler_params=pltpu.CompilerParams(vmem_limit_bytes=8_000_000),
    )(sums, hot_sums, projections, widths, hot_ids)


def solution(mesh):
    placed = (
        P(("rep", "tab"), None, None),
        P("tab", "rep"),
        P("tab", None, None),
        P(),
        P("tab", None),
    )
    return jax.shard_map(
        shards,
        mesh=mesh,
        in_specs=placed,
        out_specs=(P("rep", "tab", None, None), P("tab", "rep", None)),
        check_vma=False,
    )
```
